32 devices in a mesh: group: 2 (over y), fsdp: 16 (over z, x, core).
Axes of the slice: x: 2, y: 2, z: 4, core: 2. Of those that a mesh axis runs over, the one named last changes fastest.
Arguments:
- teacher_rows: bfloat16 [20480, 2048], P(('group', 'fsdp')), may hold values from -6 to 6
- student_rows: bfloat16 [20480, 1024], P(('group', 'fsdp')), may hold values from -6 to 6
- counts: int32 [32], P(('group', 'fsdp')), may hold values from 213 to 640, as said below
- teacher_weight: bfloat16 [2048, 4096], P(None, ('group', 'fsdp')), may hold values from -0.125 to 0.125
- teacher_bias: float32 [4096], replicated, may hold values from -6 to 6
- teacher_gain: float32 [4096], replicated, may hold values from 0.1 to 1.9
- teacher_head: float32 [4096], replicated, may hold values from -0.09375 to 0.09375
- cross_weight: bfloat16 [1024, 1024], replicated, may hold values from -0.1875 to 0.1875
- cross_bias: float32 [1024], replicated, may hold values from -3 to 3
- out_weight: float32 [1024], replicated, may hold values from -0.1875 to 0.1875
Outputs:
- grad_cross: float32 [1024, 1024], P('fsdp')
- grad_bias: float32 [1024], replicated
- grad_out: float32 [1024], replicated
The draws below stay inside these ranges and needn't reach their ends.
Inputs may be any that keep to these rules, and one draw needn't show every extreme that they name: counts[i] live impressions fill the first slots of shard i, the rest of its 640 slots are padding.
All inputs are finite; a program needn't handle non-finite values.
Results may differ from the reference program's by a relative error of at most 0.00035.
The reference program's roundings to bfloat16 on the way (of `dcross_half`) count: a program that leaves them out, or rounds other values in their place, can miss the bound.
Values may be sent and summed in bfloat16 or wider, within the bound.
A program may use at most 128 MiB of HBM per device.

```python
import math
import jax
import jax.numpy as jnp
from jax import lax

FIN = 2048
DT = 4096
DS = 1024
ROWS_DEV = 640
SHARDS = 32
IMPR = 20480
N_GROUP = 2
N_FSDP = 16


def draw_counts(key, part):
    lowest = ROWS_DEV // 3
    spread = max(ROWS_DEV // 8, 1)
    position = jnp.arange(SHARDS, dtype=jnp.int32)
    trend = lowest + (ROWS_DEV - lowest) * position // max(SHARDS - 1, 1)
    jitter = jax.random.randint(key, (SHARDS,), -spread, spread + 1, dtype=jnp.int32)
    values = jnp.clip(trend + jitter, lowest, ROWS_DEV)
    values = values.at[0].set(lowest)
    values = values.at[SHARDS - 1].set(ROWS_DEV)
    return values.astype(jnp.int32)


def strengthened(array, stream_key, source, target, parts, factor):
    owner, partner = [(jnp.arange(array.shape[dim]) // (array.shape[dim] // parts)).reshape([-1 if axis == dim else 1 for axis in range(array.ndim)]) for dim in (source, target)]
    chosen = jax.random.permutation(stream_key, parts)[partner]
    strong = (owner == chosen) | (owner == (partner + parts // 2) % parts)
    return jnp.where(strong, factor * array, array)


def shard_levels(stream_key, extent, shards, smallest, largest):
    def one(axis_at, shards_of):
        steps = jax.random.uniform(jax.random.fold_in(jax.random.fold_in(stream_key, 6), axis_at), (shards_of,), jnp.float32, smallest / len(shards), largest / len(shards))
        return jnp.repeat(jnp.exp(steps), extent[axis_at] // shards_of).reshape((-1,) + (1,) * (len(extent) - axis_at - 1))

    level = one(*shards[0])
    for cut in shards[1:]:
        level = level * one(*cut)
    return level


def gaussian(stream_key, dims, deviation, most, split=(), held_as=jnp.bfloat16):
    values = jax.random.normal(stream_key, dims, jnp.float32) * deviation
    if len(split) > 0:
        values = shard_levels(stream_key, dims, split, -0.22, 0.18) * values
    return jnp.clip(values, min=-most, max=most).astype(held_as)


def heavy_noise(rng, extent, width, reach, cuts, heavy, kind=jnp.bfloat16):
    result = width * jax.random.normal(rng, extent, jnp.float32)
    if cuts:
        result = result * shard_levels(rng, extent, cuts, -0.22, 0.18)
    return jnp.clip(strengthened(result, jax.random.fold_in(rng, 3), *heavy), -reach, reach).astype(kind)


def setup_inputs(seed: int = 0) -> dict:
    keys = jax.random.split(jax.random.key(seed), 11)
    return {
        "teacher_rows": gaussian(keys[0], (IMPR, FIN), 1.0, 6.0, ((0, 32),)),
        "student_rows": heavy_noise(keys[1], (IMPR, DS), 1.0, 6.0, ((0, 32),), (0, 1, 32, 2.75)),
        "counts": draw_counts(jax.random.fold_in(keys[10], 71), 0),
        "teacher_weight": gaussian(keys[3], (FIN, DT), FIN ** -0.5, 0.125, ((1, 32),)),
        "teacher_bias": gaussian(keys[4], (DT,), 1.0, 6.0, (), jnp.float32),
        "teacher_gain": jnp.clip(1.0 + 0.18 * jax.random.normal(keys[5], (DT,), jnp.float32), 0.1, 1.9),
        "teacher_head": gaussian(keys[6], (DT,), DT ** -0.5, 0.09375, (), jnp.float32),
        "cross_weight": gaussian(keys[7], (DS, DS), DS ** -0.5, 0.1875),
        "cross_bias": gaussian(keys[8], (DS,), 0.5, 3.0, (), jnp.float32),
        "out_weight": gaussian(keys[9], (DS,), DS ** -0.5, 0.1875, (), jnp.float32),
    }


epsilon = 1e-06

def local_terms(rows_t, rows_s, amount, teacher_weight, teacher_bias, teacher_gain, teacher_head, cross_weight, cross_bias, out_weight, loss_scale):
    preact = jnp.dot(rows_t, teacher_weight, preferred_element_type=jnp.float32) + teacher_bias
    meansq = lax.optimization_barrier(jnp.mean(preact * preact, axis=-1, keepdims=True))
    normed = preact * lax.rsqrt(meansq + epsilon) * teacher_gain
    teacher_logit = lax.optimization_barrier(jnp.sum(jax.nn.silu(normed) * teacher_head, axis=-1))
    cross = jnp.dot(rows_s, cross_weight, preferred_element_type=jnp.float32) + cross_bias
    inputs_f = rows_s.astype(jnp.float32)
    mixed = inputs_f * cross + inputs_f
    student_logit = lax.optimization_barrier(jnp.sum(mixed * out_weight, axis=-1))
    live_rows = (jnp.arange(rows_t.shape[0], dtype=jnp.int32) < amount).astype(jnp.float32)
    error = (student_logit - teacher_logit) * live_rows * loss_scale
    dcross = error[:, None] * out_weight[None, :] * inputs_f
    dcross_half = dcross.astype(jnp.bfloat16)
    term_w = lax.dot_general(rows_s, dcross_half, (((0,), (0,)), ((), ())), preferred_element_type=jnp.float32)
    term_b = lax.optimization_barrier(jnp.sum(dcross, axis=0))
    term_o = lax.optimization_barrier(jnp.sum(error[:, None] * mixed, axis=0))
    return (term_w, term_b, term_o)

def reference(teacher_rows, student_rows, counts, teacher_weight, teacher_bias, teacher_gain, teacher_head, cross_weight, cross_bias, out_weight):
    shard_count = N_GROUP * N_FSDP
    loss_scale = math.sqrt(DS / (ROWS_DEV * shard_count))
    blocks_t = teacher_rows.reshape(shard_count, ROWS_DEV, FIN)
    blocks_s = student_rows.reshape(shard_count, ROWS_DEV, DS)

    def visit(carry, inputs):
        rows_t, rows_s, amount = inputs
        terms = local_terms(rows_t, rows_s, amount, teacher_weight, teacher_bias, teacher_gain, teacher_head, cross_weight, cross_bias, out_weight, loss_scale)
        return ((carry[0] + terms[0], carry[1] + terms[1], carry[2] + terms[2]), None)
    start_sums = (jnp.zeros((DS, DS), jnp.float32), jnp.zeros((DS,), jnp.float32), jnp.zeros((DS,), jnp.float32))
    totals, unused = lax.scan(visit, start_sums, (blocks_t, blocks_s, counts))
    return (totals[0], totals[1], totals[2])
```

```python
import functools
import math

import jax
import jax.numpy as jnp
from jax import lax
from jax.experimental import pallas as pl
from jax.experimental.pallas import tpu as pltpu
from jax.sharding import PartitionSpec as P

epsilon = 1e-06


def shards(
    teacher_rows,
    student_rows,
    counts,
    teacher_weight,
    teacher_bias,
    teacher_gain,
    teacher_head,
    cross_weight,
    cross_bias,
    out_weight,
):
    row_count = teacher_rows.shape[0]
    width_s = cross_weight.shape[0]
    group_count = lax.axis_size("group")
    fsdp_count = lax.axis_size("fsdp")
    shard_count = group_count * fsdp_count
    loss_scale = math.sqrt(width_s / (row_count * shard_count))
    preact = jnp.dot(
        teacher_rows,
        lax.all_gather(teacher_weight, ("group", "fsdp"), axis=1, tiled=True),
        preferred_element_type=jnp.float32,
    )
    preact = preact + teacher_bias
    meansq = jnp.mean(preact * preact, axis=-1, keepdims=True)
    normed = preact * lax.rsqrt(meansq + epsilon) * teacher_gain
    teacher_logit = jnp.sum(jax.nn.silu(normed) * teacher_head, axis=-1)
    cross = jnp.dot(student_rows, cross_weight, preferred_element_type=jnp.float32) + cross_bias
    inputs_f = student_rows.astype(jnp.float32)
    mixed = inputs_f * cross + inputs_f
    student_logit = jnp.sum(mixed * out_weight, axis=-1)
    live_rows = (jnp.arange(row_count, dtype=jnp.int32) < counts[0]).astype(jnp.float32)
    error = (student_logit - teacher_logit) * live_rows * loss_scale
    dcross = error[:, None] * out_weight[None, :] * inputs_f
    dcross_half = dcross.astype(jnp.bfloat16)
    term_b = jnp.sum(dcross, axis=0)
    term_o = jnp.sum(error[:, None] * mixed, axis=0)
    term_w = lax.dot_general(
        student_rows, dcross_half, (((0,), (0,)), ((), ())), preferred_element_type=jnp.float32
    )
    totals = lax.psum((term_w, term_b, term_o), "group")
    grad_cross = lax.psum_scatter(totals[0], "fsdp", scatter_dimension=0, tiled=True)
    small_sums = lax.psum((totals[1], totals[2]), "fsdp")
    return (grad_cross, small_sums[0], small_sums[1])


MESH = pl.DeviceIdType.MESH
LANES = 128
PAIRS = 4
QUARTERS = 4


def fused(fsdp_count, rp, t_ref, s_ref, live_ref, w_ref, bias_ref, gain_ref, head_ref, cw_ref, cb_ref, ow_ref,
          out_ref, small_ref,
          wbuf, rows, xs, cw, pre, ssq, gains, heads, mixed, msg1, in1, msg2, in2, rr, er, xt, dbuf,
          tw, r1, s1, r2, tt, r3, fin, r4, sb, rb, rz, lsem, ssem, rsem, wsem):
    g = lax.axis_index("group")
    f = lax.axis_index("fsdp")
    core = lax.rem(f, 2)
    x = lax.rem(lax.div(f, 2), 2)
    z = lax.div(f, 4)
    nz = fsdp_count // 4
    row_count, fin_width = t_ref.shape
    width_s = s_ref.shape[1]
    block = width_s // fsdp_count
    half_rows = block // 2
    rt = row_count // LANES
    units = bias_ref.shape[0] * LANES
    parts = 2 * PAIRS
    pw = width_s // parts

    def at(y_, z_, x_, c_):
        return (y_, (z_ * 2 + x_) * 2 + c_)

    partner = at(g, z, x, 1 - core)
    xn = at(g, z, 1 - x, core)
    yn = at(1 - g, z, x, core)
    barrier = pltpu.get_barrier_semaphore()
    peers = [partner, xn, yn] + [at(g, lax.rem(z + k, nz), x, core) for k in range(1, nz)]
    for peer in peers:
        pl.semaphore_signal(barrier, inc=1, device_id=peer, device_id_type=MESH)

    locals_ = []
    for i, (a, b) in enumerate([
        (s_ref, xs.at[pl.ds(0, row_count)]),
        (cw_ref, cw),
        (w_ref, wbuf.at[0]),
        (t_ref, rows.at[pl.ds(0, row_count)]),
    ]):
        cp = pltpu.make_async_copy(a, b, lsem.at[i])
        cp.start()
        locals_.append(cp)
    pl.semaphore_wait(barrier, len(peers))

    sends = []
    mid_sends = []
    waits = []
    turn = [0]

    def send(a, b, device, recv=None, only_mid=False):
        i = turn[0]
        turn[0] += 1
        if recv is None:
            recv = rsem.at[len(waits)]
            waits.append(i)
        cp = pltpu.make_async_remote_copy(
            src_ref=a, dst_ref=b, send_sem=ssem.at[i], recv_sem=recv, device_id=device, device_id_type=MESH
        )
        cp.start()
        if only_mid:
            mid_sends.append(i)
        else:
            sends.append(cp)
        return cp

    half_z = lax.div(z, 2)
    is_mid = jnp.logical_or(z == 1, z == 2)
    is_end = jnp.logical_not(is_mid)
    plane = (z, z + 1 - 2 * lax.rem(z, 2), 2 - half_z, 3 - 3 * half_z)
    zpair = at(g, plane[1], x, core)
    zmid = at(g, nz - 1 - z, x, core)
    depth = fin_width // QUARTERS
    quarters = list(range(QUARTERS))
    first, last = quarters[:QUARTERS // 2], quarters[QUARTERS // 2:]

    def slot(dx, dy, n):
        return (dx * 2 + dy) * nz + n

    def piece(dx, dy, n, q):
        return wbuf.at[slot(dx, dy, n), pl.ds(q * depth, depth)]

    def arrival(dx, dy, n, q):
        return wsem.at[slot(dx, dy, n) * QUARTERS + q]

    def pass_on(src, dst, q, device, only_mid=False):
        here = w_ref.at[pl.ds(q * depth, depth)] if src is None else piece(*src, q)
        send(here, piece(*dst, q), device, arrival(*dst, q), only_mid)

    def landed(dx, dy, n, qs):
        for q in qs:
            pltpu.make_async_remote_copy(
                src_ref=piece(dx, dy, n, q), dst_ref=piece(dx, dy, n, q), send_sem=ssem.at[0],
                recv_sem=arrival(dx, dy, n, q), device_id=partner, device_id_type=MESH
            ).wait_recv()

    def sideways(src, n):
        for qx, qy in zip(last + first, quarters):
            pass_on(src, (1, 0, n), qx, xn)
            pass_on(src, (0, 1, n), qy, yn)

    for qx, q in zip(last + first, quarters):
        pass_on(None, (1, 0, 0), qx, xn)
        pass_on(None, (0, 1, 0), q, yn)
        pass_on(None, (0, 0, 1), q, zpair)

    @pl.when(is_mid)
    def _():
        for q in quarters:
            pass_on(None, (0, 0, 2), q, zmid, True)

    rows_in = send(t_ref, rows.at[pl.ds(row_count, row_count)], partner)
    xs_in = send(s_ref, xs.at[pl.ds(row_count, row_count)], partner)

    def diagonal(n):
        for qx, qy in zip(first, last):
            landed(0, 1, n, [qx])
            pass_on((0, 1, n), (1, 1, n), qx, xn)
            landed(1, 0, n, [qy])
            pass_on((1, 0, n), (1, 1, n), qy, yn)

    def rest(n):
        landed(0, 1, n, last)
        landed(1, 0, n, first)

    eye = lax.broadcasted_iota(jnp.int32, (LANES, LANES), 0) == lax.broadcasted_iota(jnp.int32, (LANES, LANES), 1)

    def to_row(col):
        return jnp.sum(jnp.where(eye, col, 0.0), axis=0, keepdims=True)

    def to_col(row):
        return jnp.sum(jnp.where(eye, row, 0.0), axis=1, keepdims=True)

    def tile(t):
        return pl.ds(pl.multiple_of(t * LANES, LANES), LANES)

    ssq[...] = jnp.zeros_like(ssq)
    for ref in (msg1, msg2, er, rr):
        ref[...] = jnp.zeros_like(ref)
    msg1[pl.ds(3 * rp, rt), :] = live_ref[...]

    locals_[0].wait()
    locals_[1].wait()
    ow = ow_ref[...]

    def student(t, carry):
        xt_ = xs[tile(t), :]
        cross = jnp.dot(xt_, cw[...], preferred_element_type=jnp.float32) + cb_ref[...]
        xf = xt_.astype(jnp.float32)
        m = xf * cross + xf
        mixed[tile(t), :] = m
        msg1[pl.ds(2 * rp + t, 1), :] = to_row(jnp.sum(m * ow, axis=1, keepdims=True))
        return carry

    lax.fori_loop(0, rt, student, 0)
    locals_[2].wait()
    locals_[3].wait()

    mt = row_count

    def project(dx, dy, n):
        s = slot(dx, dy, n)
        y_ = g if dy == 0 else 1 - g
        x_ = x if dx == 0 else 1 - x
        index = y_ * fsdp_count + (plane[n] * 2 + x_) * 2 + core
        gains[pl.ds(s, 1), :] = gain_ref[index] * 0.5
        heads[pl.ds(s, 1), :] = head_ref[index]
        bias = bias_ref[index]

        def step(t, carry):
            ds = pl.ds(pl.multiple_of(t * mt, mt), mt)
            p = jnp.dot(rows[ds, :], wbuf[s], preferred_element_type=jnp.float32) + bias
            pre[s, ds, :] = p
            ssq[ds, :] += p * p
            return carry

        lax.fori_loop(0, 2 * row_count // mt, step, 0)

    rows_in.wait_recv()
    project(0, 0, 0)
    diagonal(0)

    @pl.when(is_mid)
    def _():
        for q in quarters:
            landed(0, 0, 2, [q])
            pass_on((0, 0, 2), (0, 0, 2), q, zpair, True)

    for q in quarters:
        landed(0, 0, 1, [q])

        @pl.when(is_mid)
        def _(q=q):
            pass_on((0, 0, 1), (0, 0, 3), q, zmid, True)

    sideways((0, 0, 1), 1)
    rest(0)
    project(1, 0, 0)
    project(0, 1, 0)
    project(0, 0, 1)
    for q in [q for pair in zip(first, last) for q in pair]:
        landed(1, 1, 0, [q])
        pass_on((1, 1, 0), (1, 1, 1), q, zpair)

        @pl.when(is_mid)
        def _(q=q):
            pass_on((1, 1, 0), (1, 1, 2), q, zmid, True)

    xs_in.wait_recv()
    pick = (
        lax.broadcasted_iota(jnp.int32, (block, 2 * block), 1)
        == lax.broadcasted_iota(jnp.int32, (block, 2 * block), 0) + core * block
    )
    pick = jnp.where(pick, 1.0, 0.0).astype(jnp.bfloat16)
    for j in range(fsdp_count // 2):
        xt[pl.ds(j * block, block), :] = lax.dot_general(
            pick, xs[:, pl.ds(j * 2 * block, 2 * block)], (((1,), (1,)), ((), ())), preferred_element_type=jnp.float32
        ).astype(jnp.bfloat16)

    @pl.when(is_mid)
    def _():
        for q in quarters:
            landed(0, 0, 3, [q])
            pass_on((0, 0, 3), (0, 0, 3), q, zpair, True)

    project(1, 1, 0)

    @pl.when(is_end)
    def _():
        landed(0, 0, 2, quarters)

    sideways((0, 0, 2), 2)
    project(0, 0, 2)
    for at_ in ((1, 0, 1), (0, 1, 1)):
        landed(*at_, quarters)
        project(*at_)

    @pl.when(is_end)
    def _():
        landed(0, 0, 3, quarters)

    sideways((0, 0, 3), 3)

    @pl.when(is_mid)
    def _():
        for q in quarters:
            landed(1, 1, 2, [q])
            pass_on((1, 1, 2), (1, 1, 2), q, zpair, True)

    project(0, 0, 3)
    for at_ in ((1, 0, 2), (0, 1, 2)):
        landed(*at_, quarters)
        project(*at_)
    diagonal(3)
    landed(1, 1, 1, quarters)
    project(1, 1, 1)
    rest(3)
    project(1, 0, 3)
    project(0, 1, 3)

    @pl.when(is_end)
    def _():
        landed(1, 1, 2, quarters)

    project(1, 1, 2)
    landed(1, 1, 3, quarters)
    project(1, 1, 3)

    for h in range(2):
        def squares(t, carry, h=h):
            col = jnp.sum(ssq[tile(h * rt + t), :], axis=1, keepdims=True)
            msg1[pl.ds(h * rp + t, 1), :] = to_row(col)
            return carry

        lax.fori_loop(0, rt, squares, 0)
    m1 = send(msg1, in1, partner)
    m1.wait_recv()
    for h in range(2):
        total = msg1[pl.ds(h * rp, rp), :] + in1[pl.ds((1 - h) * rp, rp), :]
        rr[pl.ds(h * rp, rp), :] = lax.rsqrt(total * (1.0 / units) + epsilon)

    for h in range(2):
        def logits(t, carry, h=h):
            r = to_col(rr[pl.ds(h * rp + t, 1), :])
            acc = jnp.zeros((LANES, LANES), jnp.float32)
            for s in range(4 * nz):
                v = pre[s, tile(h * rt + t), :] * r * gains[pl.ds(s, 1), :]
                acc += (v * jnp.tanh(v) + v) * heads[pl.ds(s, 1), :]
            msg2[pl.ds(h * rp + t, 1), :] = to_row(jnp.sum(acc, axis=1, keepdims=True))
            return carry

        lax.fori_loop(0, rt, logits, 0)
    m2 = send(msg2, in2, partner)
    m2.wait_recv()
    for h, src in ((0, msg1), (1, in1)):
        teacher = msg2[pl.ds(h * rp, rp), :] + in2[pl.ds((1 - h) * rp, rp), :]
        er[pl.ds(h * rp, rp), :] = (src[pl.ds(2 * rp, rp), :] - teacher) * src[pl.ds(3 * rp, rp), :]

    sb[...] = jnp.zeros_like(sb)

    def own(t, carry):
        e = to_col(er[pl.ds(t, 1), :])
        d = e * ow * xs[tile(t), :].astype(jnp.float32)
        dbuf[tile(t), :] = d.astype(jnp.bfloat16)
        sb[0, pl.ds(0, 1), :] += jnp.sum(d, axis=0, keepdims=True)
        sb[0, pl.ds(1, 1), :] += jnp.sum(e * mixed[tile(t), :], axis=0, keepdims=True)
        return carry

    lax.fori_loop(0, rt, own, 0)
    c0 = send(sb.at[0], rb.at[0], partner)

    def other(t, carry):
        e = to_col(er[pl.ds(rp + t, 1), :])
        d = e * ow * xs[tile(rt + t), :].astype(jnp.float32)
        dbuf[tile(rt + t), :] = d.astype(jnp.bfloat16)
        return carry

    lax.fori_loop(0, rt, other, 0)

    def way(p):
        return (g, x, yn, xn) if p % 2 == 0 else (x, g, xn, yn)

    h1, h2, h3, h4 = {}, {}, {}, {}

    def stage1(p):
        val = jnp.dot(xt[...], dbuf[:, pl.ds(p * pw, pw)], preferred_element_type=jnp.float32)
        for z_ in range(nz):
            for x_ in range(2):
                for y_ in range(2):
                    first, second = (y_, x_) if p % 2 == 0 else (x_, y_)
                    offset = ((z_ * 2 + x_) * 2 + y_) * half_rows
                    tw[p, first, second, z_] = val[offset:offset + half_rows, :]
        first, second, n1, n2 = way(p)
        h1[p] = send(tw.at[p, 1 - first], r1.at[p], n1)

    def stage2(p):
        first, second, n1, n2 = way(p)
        h1[p].wait_recv()
        s1[p] = tw[p, first] + r1[p]
        h2[p] = send(s1.at[p, 1 - second], r2.at[p], n2)

    def stage3(p):
        first, second, n1, n2 = way(p)
        h2[p].wait_recv()
        tt[p] = s1[p, second] + r2[p]
        h3[p] = []
        for k in range(1, nz):
            to = lax.rem(z + k, nz)
            h3[p].append(send(tt.at[p, to], r3.at[p, k - 1], at(g, to, x, core)))

    def stage4(p):
        total = tt[p, z]
        for k in range(nz - 1):
            h3[p][k].wait_recv()
            total = total + r3[p, k]
        fin[p] = total
        h4[p] = send(fin.at[p], r4.at[p], yn)
        out_ref[pl.ds(pl.multiple_of(g * half_rows, half_rows), half_rows), pl.ds(p * pw, pw)] = total

    cz = []

    def small(n):
        if n == 0:
            c0.wait_recv()
            sb[1] = sb[0] + rb[0]
            cz.append(send(sb.at[1], rb.at[1], xn))
        elif n == 1:
            cz.pop().wait_recv()
            sb[2] = sb[1] + rb[1]
            cz.append(send(sb.at[2], rb.at[2], yn))
        elif n == 2:
            cz.pop().wait_recv()
            sb[3] = sb[2] + rb[2]
            rz[z] = sb[3]
            for k in range(1, nz):
                to = lax.rem(z + k, nz)
                cz.append(send(sb.at[3], rz.at[z], at(g, to, x, core)))

    stages = (stage1, stage2, stage3, stage4)
    lag = (0, 2, 3, 5)
    for step in range(PAIRS + lag[-1]):
        for stage, behind in zip(stages, lag):
            q = step - behind
            if 0 <= q < PAIRS:
                stage(2 * q)
                stage(2 * q + 1)
        small(step - 1)
    for cp in cz:
        cp.wait_recv()
    total = rz[0]
    for k in range(1, nz):
        total = total + rz[k]
    small_ref[...] = total
    for p in range(parts):
        h4[p].wait_recv()
        out_ref[pl.ds(pl.multiple_of((1 - g) * half_rows, half_rows), half_rows), pl.ds(p * pw, pw)] = r4[p]
    for cp in sends:
        cp.wait_send()

    @pl.when(is_mid)
    def _():
        for i in mid_sends:
            pltpu.make_async_remote_copy(
                src_ref=piece(0, 0, 0, 0), dst_ref=piece(0, 0, 0, 0), send_sem=ssem.at[i], recv_sem=wsem.at[0],
                device_id=partner, device_id_type=MESH
            ).wait_send()


def shards_fused(
    teacher_rows,
    student_rows,
    counts,
    teacher_weight,
    teacher_bias,
    teacher_gain,
    teacher_head,
    cross_weight,
    cross_bias,
    out_weight,
):
    row_count, fin_width = teacher_rows.shape
    width_s = cross_weight.shape[0]
    group_count = lax.axis_size("group")
    fsdp_count = lax.axis_size("fsdp")
    loss_scale = math.sqrt(width_s / (row_count * group_count * fsdp_count))
    live = (jnp.arange(row_count, dtype=jnp.int32) < counts[0]).astype(jnp.float32) * loss_scale
    rt = row_count // LANES
    rp = -(-rt // 8) * 8
    nz = fsdp_count // 4
    block = width_s // fsdp_count
    half_rows = block // 2
    parts = 2 * PAIRS
    pw = width_s // parts
    slots = 4 * nz
    f32, bf16 = jnp.float32, jnp.bfloat16
    vm = pltpu.VMEM
    split = lambda v: v.reshape(-1, 1, LANES)
    anyspec = pl.BlockSpec(memory_space=pl.ANY)
    vspec = pl.BlockSpec(memory_space=pltpu.VMEM)
    grad, small = pl.pallas_call(
        functools.partial(fused, fsdp_count, rp),
        out_shape=(jax.ShapeDtypeStruct((block, width_s), f32), jax.ShapeDtypeStruct((8, width_s), f32)),
        in_specs=[anyspec, anyspec, vspec, anyspec, vspec, vspec, vspec, anyspec, vspec, vspec],
        out_specs=(vspec, vspec),
        scratch_shapes=[
            vm((slots, fin_width, LANES), bf16),
            vm((2 * row_count, fin_width), bf16),
            vm((2 * row_count, width_s), bf16),
            vm((width_s, width_s), bf16),
            vm((slots, 2 * row_count, LANES), f32),
            vm((2 * row_count, LANES), f32),
            vm((slots, LANES), f32),
            vm((slots, LANES), f32),
            vm((row_count, width_s), f32),
            vm((4 * rp, LANES), f32),
            vm((4 * rp, LANES), f32),
            vm((2 * rp, LANES), f32),
            vm((2 * rp, LANES), f32),
            vm((2 * rp, LANES), f32),
            vm((2 * rp, LANES), f32),
            vm((width_s // 2, 2 * row_count), bf16),
            vm((2 * row_count, width_s), bf16),
            vm((parts, 2, 2, nz, half_rows, pw), f32),
            vm((parts, 2, nz, half_rows, pw), f32),
            vm((parts, 2, nz, half_rows, pw), f32),
            vm((parts, nz, half_rows, pw), f32),
            vm((parts, nz, half_rows, pw), f32),
            vm((parts, nz - 1, half_rows, pw), f32),
            vm((parts, half_rows, pw), f32),
            vm((parts, half_rows, pw), f32),
            vm((4, 8, width_s), f32),
            vm((3, 8, width_s), f32),
            vm((nz, 8, width_s), f32),
            pltpu.SemaphoreType.DMA((4,)),
            pltpu.SemaphoreType.DMA((SENDS,)),
            pltpu.SemaphoreType.DMA((OTHERS,)),
            pltpu.SemaphoreType.DMA((slots * QUARTERS,)),
        ],
        compiler_params=pltpu.CompilerParams(
            collective_id=0, has_side_effects=True, vmem_limit_bytes=60 * 1024 * 1024
        ),
    )(
        teacher_rows, student_rows, live.reshape(rt, LANES), teacher_weight, split(teacher_bias), split(teacher_gain),
        split(teacher_head), cross_weight, cross_bias[None, :], out_weight[None, :],
    )
    return (grad, small[0], small[1])


SENDS = 160
OTHERS = 72


def fits(mesh, args):
    rows, fin_width = args[0].shape
    width_s = args[1].shape[1]
    units = args[3].shape[1]
    group_count, fsdp_count = mesh.shape["group"], mesh.shape["fsdp"]
    devices = group_count * fsdp_count
    return (
        group_count == 2
        and fsdp_count == 16
        and units == devices * LANES
        and (rows // devices) % LANES == 0
        and (2 * width_s // fsdp_count) % LANES == 0
        and width_s % (2 * PAIRS * LANES) == 0
    )


def solution(mesh):
    in_specs = (
        P(("group", "fsdp"), None),
        P(("group", "fsdp"), None),
        P(("group", "fsdp")),
        P(None, ("group", "fsdp")),
        P(),
        P(),
        P(),
        P(),
        P(),
        P(),
    )
    out_specs = (P("fsdp", None), P(), P())

    def run(*args):
        body = shards_fused if fits(mesh, args) else shards
        return jax.shard_map(body, mesh=mesh, in_specs=in_specs, out_specs=out_specs, check_vma=False)(*args)

    return run
```

```python
import functools
import math

import jax
import jax.numpy as jnp
from jax import lax
from jax.experimental import pallas as pl
from jax.experimental.pallas import tpu as pltpu
from jax.sharding import PartitionSpec as P

epsilon = 1e-06


def shards(
    teacher_rows,
    student_rows,
    counts,
    teacher_weight,
    teacher_bias,
    teacher_gain,
    teacher_head,
    cross_weight,
    cross_bias,
    out_weight,
):
    row_count = teacher_rows.shape[0]
    width_s = cross_weight.shape[0]
    group_count = lax.axis_size("group")
    fsdp_count = lax.axis_size("fsdp")
    shard_count = group_count * fsdp_count
    loss_scale = math.sqrt(width_s / (row_count * shard_count))
    preact = jnp.dot(
        teacher_rows,
        lax.all_gather(teacher_weight, ("group", "fsdp"), axis=1, tiled=True),
        preferred_element_type=jnp.float32,
    )
    preact = preact + teacher_bias
    meansq = jnp.mean(preact * preact, axis=-1, keepdims=True)
    normed = preact * lax.rsqrt(meansq + epsilon) * teacher_gain
    teacher_logit = jnp.sum(jax.nn.silu(normed) * teacher_head, axis=-1)
    cross = jnp.dot(student_rows, cross_weight, preferred_element_type=jnp.float32) + cross_bias
    inputs_f = student_rows.astype(jnp.float32)
    mixed = inputs_f * cross + inputs_f
    student_logit = jnp.sum(mixed * out_weight, axis=-1)
    live_rows = (jnp.arange(row_count, dtype=jnp.int32) < counts[0]).astype(jnp.float32)
    error = (student_logit - teacher_logit) * live_rows * loss_scale
    dcross = error[:, None] * out_weight[None, :] * inputs_f
    dcross_half = dcross.astype(jnp.bfloat16)
    term_b = jnp.sum(dcross, axis=0)
    term_o = jnp.sum(error[:, None] * mixed, axis=0)
    term_w = lax.dot_general(
        student_rows, dcross_half, (((0,), (0,)), ((), ())), preferred_element_type=jnp.float32
    )
    totals = lax.psum((term_w, term_b, term_o), "group")
    grad_cross = lax.psum_scatter(totals[0], "fsdp", scatter_dimension=0, tiled=True)
    small_sums = lax.psum((totals[1], totals[2]), "fsdp")
    return (grad_cross, small_sums[0], small_sums[1])


MESH = pl.DeviceIdType.MESH
LANES = 128
PAIRS = 4
QUARTERS = 4


def fused(fsdp_count, rp, t_ref, s_ref, live_ref, w_ref, bias_ref, gain_ref, head_ref, cw_ref, cb_ref, ow_ref,
          out_ref, small_ref,
          wbuf, rows, xs, cw, pre, ssq, gains, heads, mixed, msg1, in1, msg2, in2, rr, er, xt, dbuf,
          tw, r1, s1, r2, tt, r3, fin, r4, sb, rb, rz, lsem, ssem, rsem, wsem):
    g = lax.axis_index("group")
    f = lax.axis_index("fsdp")
    core = lax.rem(f, 2)
    x = lax.rem(lax.div(f, 2), 2)
    z = lax.div(f, 4)
    nz = fsdp_count // 4
    row_count, fin_width = t_ref.shape
    width_s = s_ref.shape[1]
    block = width_s // fsdp_count
    half_rows = block // 2
    rt = row_count // LANES
    units = bias_ref.shape[0] * LANES
    parts = 2 * PAIRS
    pw = width_s // parts

    def at(y_, z_, x_, c_):
        return (y_, (z_ * 2 + x_) * 2 + c_)

    partner = at(g, z, x, 1 - core)
    xn = at(g, z, 1 - x, core)
    yn = at(1 - g, z, x, core)
    barrier = pltpu.get_barrier_semaphore()
    peers = [partner, xn, yn] + [at(g, lax.rem(z + k, nz), x, core) for k in range(1, nz)]
    for peer in peers:
        pl.semaphore_signal(barrier, inc=1, device_id=peer, device_id_type=MESH)

    locals_ = []
    for i, (a, b) in enumerate([
        (s_ref, xs.at[pl.ds(0, row_count)]),
        (cw_ref, cw),
        (w_ref, wbuf.at[0]),
        (t_ref, rows.at[pl.ds(0, row_count)]),
    ]):
        cp = pltpu.make_async_copy(a, b, lsem.at[i])
        cp.start()
        locals_.append(cp)
    pl.semaphore_wait(barrier, len(peers))

    sends = []
    mid_sends = []
    end_sends = []
    waits = []
    turn = [0]

    def send(a, b, device, recv=None, only=None):
        i = turn[0]
        turn[0] += 1
        if recv is None:
            recv = rsem.at[len(waits)]
            waits.append(i)
        cp = pltpu.make_async_remote_copy(
            src_ref=a, dst_ref=b, send_sem=ssem.at[i], recv_sem=recv, device_id=device, device_id_type=MESH
        )
        cp.start()
        if only:
            (end_sends if only == 'end' else mid_sends).append(i)
        else:
            sends.append(cp)
        return cp

    half_z = lax.div(z, 2)
    is_mid = jnp.logical_or(z == 1, z == 2)
    is_end = jnp.logical_not(is_mid)
    plane = (z, z + 1 - 2 * lax.rem(z, 2), 2 - half_z, 3 - 3 * half_z)
    zpair = at(g, plane[1], x, core)
    zmid = at(g, nz - 1 - z, x, core)
    depth = fin_width // QUARTERS
    quarters = list(range(QUARTERS))
    first, last = quarters[:QUARTERS // 2], quarters[QUARTERS // 2:]

    def slot(dx, dy, n):
        return (dx * 2 + dy) * nz + n

    def piece(dx, dy, n, q):
        return wbuf.at[slot(dx, dy, n), pl.ds(q * depth, depth)]

    def arrival(dx, dy, n, q):
        return wsem.at[slot(dx, dy, n) * QUARTERS + q]

    def pass_on(src, dst, q, device, only=None):
        here = w_ref.at[pl.ds(q * depth, depth)] if src is None else piece(*src, q)
        send(here, piece(*dst, q), device, arrival(*dst, q), only)

    def landed(dx, dy, n, qs):
        for q in qs:
            pltpu.make_async_remote_copy(
                src_ref=piece(dx, dy, n, q), dst_ref=piece(dx, dy, n, q), send_sem=ssem.at[0],
                recv_sem=arrival(dx, dy, n, q), device_id=partner, device_id_type=MESH
            ).wait_recv()

    def sideways(src, n):
        for qx, qy in zip(last + first, quarters):
            pass_on(src, (1, 0, n), qx, xn)
            pass_on(src, (0, 1, n), qy, yn)

    for qx, q in zip(last + first, quarters):
        pass_on(None, (1, 0, 0), qx, xn)
        pass_on(None, (0, 1, 0), q, yn)
        pass_on(None, (0, 0, 1), q, zpair)

    @pl.when(is_mid)
    def _():
        for q in quarters:
            pass_on(None, (0, 0, 2), q, zmid, 'mid')

    rows_in = send(t_ref, rows.at[pl.ds(row_count, row_count)], partner)
    xs_in = send(s_ref, xs.at[pl.ds(row_count, row_count)], partner)

    def diagonal(n):
        for qx, qy in zip(first, last):
            landed(0, 1, n, [qx])
            pass_on((0, 1, n), (1, 1, n), qx, xn)
            landed(1, 0, n, [qy])
            pass_on((1, 0, n), (1, 1, n), qy, yn)

    def rest(n):
        landed(0, 1, n, last)
        landed(1, 0, n, first)

    eye = lax.broadcasted_iota(jnp.int32, (LANES, LANES), 0) == lax.broadcasted_iota(jnp.int32, (LANES, LANES), 1)

    def to_row(col):
        return jnp.sum(jnp.where(eye, col, 0.0), axis=0, keepdims=True)

    def to_col(row):
        return jnp.sum(jnp.where(eye, row, 0.0), axis=1, keepdims=True)

    def tile(t):
        return pl.ds(pl.multiple_of(t * LANES, LANES), LANES)

    ssq[...] = jnp.zeros_like(ssq)
    for ref in (msg1, msg2, er, rr):
        ref[...] = jnp.zeros_like(ref)
    msg1[pl.ds(3 * rp, rt), :] = live_ref[...]

    locals_[0].wait()
    locals_[1].wait()
    ow = ow_ref[...]

    def student(t, carry):
        xt_ = xs[tile(t), :]
        cross = jnp.dot(xt_, cw[...], preferred_element_type=jnp.float32) + cb_ref[...]
        xf = xt_.astype(jnp.float32)
        m = xf * cross + xf
        mixed[tile(t), :] = m
        msg1[pl.ds(2 * rp + t, 1), :] = to_row(jnp.sum(m * ow, axis=1, keepdims=True))
        return carry

    lax.fori_loop(0, rt, student, 0)
    locals_[2].wait()
    locals_[3].wait()

    mt = row_count

    def project(dx, dy, n):
        s = slot(dx, dy, n)
        y_ = g if dy == 0 else 1 - g
        x_ = x if dx == 0 else 1 - x
        index = y_ * fsdp_count + (plane[n] * 2 + x_) * 2 + core
        gains[pl.ds(s, 1), :] = gain_ref[index] * 0.5
        heads[pl.ds(s, 1), :] = head_ref[index]
        bias = bias_ref[index]

        def step(t, carry):
            ds = pl.ds(pl.multiple_of(t * mt, mt), mt)
            p = jnp.dot(rows[ds, :], wbuf[s], preferred_element_type=jnp.float32) + bias
            pre[s, ds, :] = p
            ssq[ds, :] += p * p
            return carry

        lax.fori_loop(0, 2 * row_count // mt, step, 0)

    order = [q for pair in zip(first, last) for q in pair]

    for i, (qx, qy) in enumerate(zip(first, last)):
        landed(0, 1, 0, [qx])
        pass_on((0, 1, 0), (1, 1, 0), qx, xn)
        landed(1, 0, 0, [qy])
        pass_on((1, 0, 0), (1, 1, 0), qy, yn)

        @pl.when(is_mid)
        def _(i=i):
            for q in quarters[2 * i:2 * i + 2]:
                landed(0, 0, 2, [q])
                pass_on((0, 0, 2), (0, 0, 2), q, zpair, 'mid')
                landed(0, 0, 1, [q])
                pass_on((0, 0, 1), (0, 0, 3), q, zmid, 'mid')

    rows_in.wait_recv()
    project(0, 0, 0)

    @pl.when(is_end)
    def _():
        landed(0, 0, 1, quarters)

    sideways((0, 0, 1), 1)
    rest(0)
    project(1, 0, 0)

    def far(q):
        landed(0, 0, 3, [q])
        pass_on((0, 0, 3), (0, 0, 3), q, zpair, 'mid')

    @pl.when(is_mid)
    def _():
        far(0)

    project(0, 1, 0)
    for i, q in enumerate(order):
        landed(1, 1, 0, [q])

        @pl.when(is_end)
        def _(q=q):
            pass_on((1, 1, 0), (1, 1, 1), q, zpair, 'end')

        @pl.when(is_mid)
        def _(q=q, i=i):
            pass_on((1, 1, 0), (1, 1, 2), q, zmid, 'mid')
            if i == 1:
                far(1)

    project(0, 0, 1)
    xs_in.wait_recv()
    pick = (
        lax.broadcasted_iota(jnp.int32, (block, 2 * block), 1)
        == lax.broadcasted_iota(jnp.int32, (block, 2 * block), 0) + core * block
    )
    pick = jnp.where(pick, 1.0, 0.0).astype(jnp.bfloat16)
    for j in range(fsdp_count // 2):
        xt[pl.ds(j * block, block), :] = lax.dot_general(
            pick, xs[:, pl.ds(j * 2 * block, 2 * block)], (((1,), (1,)), ((), ())), preferred_element_type=jnp.float32
        ).astype(jnp.bfloat16)

    @pl.when(is_mid)
    def _():
        for q in quarters[2:]:
            far(q)
        for q in order:
            pass_on((1, 1, 0), (1, 1, 1), q, zpair, 'mid')

    @pl.when(is_end)
    def _():
        landed(0, 0, 2, quarters)

    sideways((0, 0, 2), 2)
    project(1, 1, 0)
    project(0, 0, 2)
    landed(1, 0, 1, quarters)
    project(1, 0, 1)
    landed(0, 1, 1, quarters)

    @pl.when(is_end)
    def _():
        landed(0, 0, 3, quarters)

    sideways((0, 0, 3), 3)
    project(0, 1, 1)

    @pl.when(is_mid)
    def _():
        for q in order:
            landed(1, 1, 2, [q])
            pass_on((1, 1, 2), (1, 1, 2), q, zpair, 'mid')

    project(0, 0, 3)
    for at_ in ((1, 0, 2), (0, 1, 2)):
        landed(*at_, quarters)
        project(*at_)
    diagonal(3)
    landed(1, 1, 1, quarters)
    project(1, 1, 1)
    rest(3)
    project(1, 0, 3)
    project(0, 1, 3)

    @pl.when(is_end)
    def _():
        landed(1, 1, 2, quarters)

    project(1, 1, 2)
    landed(1, 1, 3, quarters)
    project(1, 1, 3)

    for h in range(2):
        def squares(t, carry, h=h):
            col = jnp.sum(ssq[tile(h * rt + t), :], axis=1, keepdims=True)
            msg1[pl.ds(h * rp + t, 1), :] = to_row(col)
            return carry

        lax.fori_loop(0, rt, squares, 0)
    m1 = send(msg1, in1, partner)
    m1.wait_recv()
    for h in range(2):
        total = msg1[pl.ds(h * rp, rp), :] + in1[pl.ds((1 - h) * rp, rp), :]
        rr[pl.ds(h * rp, rp), :] = lax.rsqrt(total * (1.0 / units) + epsilon)

    for h in range(2):
        def logits(t, carry, h=h):
            r = to_col(rr[pl.ds(h * rp + t, 1), :])
            acc = jnp.zeros((LANES, LANES), jnp.float32)
            for s in range(4 * nz):
                v = pre[s, tile(h * rt + t), :] * r * gains[pl.ds(s, 1), :]
                acc += (v * jnp.tanh(v) + v) * heads[pl.ds(s, 1), :]
            msg2[pl.ds(h * rp + t, 1), :] = to_row(jnp.sum(acc, axis=1, keepdims=True))
            return carry

        lax.fori_loop(0, rt, logits, 0)
    m2 = send(msg2, in2, partner)
    m2.wait_recv()
    for h, src in ((0, msg1), (1, in1)):
        teacher = msg2[pl.ds(h * rp, rp), :] + in2[pl.ds((1 - h) * rp, rp), :]
        er[pl.ds(h * rp, rp), :] = (src[pl.ds(2 * rp, rp), :] - teacher) * src[pl.ds(3 * rp, rp), :]

    sb[...] = jnp.zeros_like(sb)

    def own(t, carry):
        e = to_col(er[pl.ds(t, 1), :])
        d = e * ow * xs[tile(t), :].astype(jnp.float32)
        dbuf[tile(t), :] = d.astype(jnp.bfloat16)
        sb[0, pl.ds(0, 1), :] += jnp.sum(d, axis=0, keepdims=True)
        sb[0, pl.ds(1, 1), :] += jnp.sum(e * mixed[tile(t), :], axis=0, keepdims=True)
        return carry

    lax.fori_loop(0, rt, own, 0)
    c0 = send(sb.at[0], rb.at[0], partner)

    def other(t, carry):
        e = to_col(er[pl.ds(rp + t, 1), :])
        d = e * ow * xs[tile(rt + t), :].astype(jnp.float32)
        dbuf[tile(rt + t), :] = d.astype(jnp.bfloat16)
        return carry

    lax.fori_loop(0, rt, other, 0)

    def way(p):
        return (g, x, yn, xn) if p % 2 == 0 else (x, g, xn, yn)

    h1, h2, h3, h4 = {}, {}, {}, {}

    def stage1(p):
        val = jnp.dot(xt[...], dbuf[:, pl.ds(p * pw, pw)], preferred_element_type=jnp.float32)
        for z_ in range(nz):
            for x_ in range(2):
                for y_ in range(2):
                    first, second = (y_, x_) if p % 2 == 0 else (x_, y_)
                    offset = ((z_ * 2 + x_) * 2 + y_) * half_rows
                    tw[p, first, second, z_] = val[offset:offset + half_rows, :]
        first, second, n1, n2 = way(p)
        h1[p] = send(tw.at[p, 1 - first], r1.at[p], n1)

    def stage2(p):
        first, second, n1, n2 = way(p)
        h1[p].wait_recv()
        s1[p] = tw[p, first] + r1[p]
        h2[p] = send(s1.at[p, 1 - second], r2.at[p], n2)

    def stage3(p):
        first, second, n1, n2 = way(p)
        h2[p].wait_recv()
        tt[p] = s1[p, second] + r2[p]
        h3[p] = []
        for k in range(1, nz):
            to = lax.rem(z + k, nz)
            h3[p].append(send(tt.at[p, to], r3.at[p, k - 1], at(g, to, x, core)))

    def stage4(p):
        total = tt[p, z]
        for k in range(nz - 1):
            h3[p][k].wait_recv()
            total = total + r3[p, k]
        fin[p] = total
        h4[p] = send(fin.at[p], r4.at[p], yn)
        out_ref[pl.ds(pl.multiple_of(g * half_rows, half_rows), half_rows), pl.ds(p * pw, pw)] = total

    cz = []

    def small(n):
        if n == 0:
            c0.wait_recv()
            sb[1] = sb[0] + rb[0]
            cz.append(send(sb.at[1], rb.at[1], xn))
        elif n == 1:
            cz.pop().wait_recv()
            sb[2] = sb[1] + rb[1]
            cz.append(send(sb.at[2], rb.at[2], yn))
        elif n == 2:
            cz.pop().wait_recv()
            sb[3] = sb[2] + rb[2]
            rz[z] = sb[3]
            for k in range(1, nz):
                to = lax.rem(z + k, nz)
                cz.append(send(sb.at[3], rz.at[z], at(g, to, x, core)))

    stages = (stage1, stage2, stage3, stage4)
    lag = (0, 2, 3, 5)
    for step in range(PAIRS + lag[-1]):
        for stage, behind in zip(stages, lag):
            q = step - behind
            if 0 <= q < PAIRS:
                stage(2 * q)
                stage(2 * q + 1)
        small(step - 1)
    for cp in cz:
        cp.wait_recv()
    total = rz[0]
    for k in range(1, nz):
        total = total + rz[k]
    small_ref[...] = total
    for p in range(parts):
        h4[p].wait_recv()
        out_ref[pl.ds(pl.multiple_of((1 - g) * half_rows, half_rows), half_rows), pl.ds(p * pw, pw)] = r4[p]
    for cp in sends:
        cp.wait_send()

    for kind, some in ((is_mid, mid_sends), (is_end, end_sends)):
        @pl.when(kind)
        def _(some=some):
            for i in some:
                pltpu.make_async_remote_copy(
                    src_ref=piece(0, 0, 0, 0), dst_ref=piece(0, 0, 0, 0), send_sem=ssem.at[i], recv_sem=wsem.at[0],
                    device_id=partner, device_id_type=MESH
                ).wait_send()


def shards_fused(
    teacher_rows,
    student_rows,
    counts,
    teacher_weight,
    teacher_bias,
    teacher_gain,
    teacher_head,
    cross_weight,
    cross_bias,
    out_weight,
):
    row_count, fin_width = teacher_rows.shape
    width_s = cross_weight.shape[0]
    group_count = lax.axis_size("group")
    fsdp_count = lax.axis_size("fsdp")
    loss_scale = math.sqrt(width_s / (row_count * group_count * fsdp_count))
    live = (jnp.arange(row_count, dtype=jnp.int32) < counts[0]).astype(jnp.float32) * loss_scale
    rt = row_count // LANES
    rp = -(-rt // 8) * 8
    nz = fsdp_count // 4
    block = width_s // fsdp_count
    half_rows = block // 2
    parts = 2 * PAIRS
    pw = width_s // parts
    slots = 4 * nz
    f32, bf16 = jnp.float32, jnp.bfloat16
    vm = pltpu.VMEM
    split = lambda v: v.reshape(-1, 1, LANES)
    anyspec = pl.BlockSpec(memory_space=pl.ANY)
    vspec = pl.BlockSpec(memory_space=pltpu.VMEM)
    grad, small = pl.pallas_call(
        functools.partial(fused, fsdp_count, rp),
        out_shape=(jax.ShapeDtypeStruct((block, width_s), f32), jax.ShapeDtypeStruct((8, width_s), f32)),
        in_specs=[anyspec, anyspec, vspec, anyspec, vspec, vspec, vspec, anyspec, vspec, vspec],
        out_specs=(vspec, vspec),
        scratch_shapes=[
            vm((slots, fin_width, LANES), bf16),
            vm((2 * row_count, fin_width), bf16),
            vm((2 * row_count, width_s), bf16),
            vm((width_s, width_s), bf16),
            vm((slots, 2 * row_count, LANES), f32),
            vm((2 * row_count, LANES), f32),
            vm((slots, LANES), f32),
            vm((slots, LANES), f32),
            vm((row_count, width_s), f32),
            vm((4 * rp, LANES), f32),
            vm((4 * rp, LANES), f32),
            vm((2 * rp, LANES), f32),
            vm((2 * rp, LANES), f32),
            vm((2 * rp, LANES), f32),
            vm((2 * rp, LANES), f32),
            vm((width_s // 2, 2 * row_count), bf16),
            vm((2 * row_count, width_s), bf16),
            vm((parts, 2, 2, nz, half_rows, pw), f32),
            vm((parts, 2, nz, half_rows, pw), f32),
            vm((parts, 2, nz, half_rows, pw), f32),
            vm((parts, nz, half_rows, pw), f32),
            vm((parts, nz, half_rows, pw), f32),
            vm((parts, nz - 1, half_rows, pw), f32),
            vm((parts, half_rows, pw), f32),
            vm((parts, half_rows, pw), f32),
            vm((4, 8, width_s), f32),
            vm((3, 8, width_s), f32),
            vm((nz, 8, width_s), f32),
            pltpu.SemaphoreType.DMA((4,)),
            pltpu.SemaphoreType.DMA((SENDS,)),
            pltpu.SemaphoreType.DMA((OTHERS,)),
            pltpu.SemaphoreType.DMA((slots * QUARTERS,)),
        ],
        compiler_params=pltpu.CompilerParams(
            collective_id=0, has_side_effects=True, vmem_limit_bytes=60 * 1024 * 1024
        ),
    )(
        teacher_rows, student_rows, live.reshape(rt, LANES), teacher_weight, split(teacher_bias), split(teacher_gain),
        split(teacher_head), cross_weight, cross_bias[None, :], out_weight[None, :],
    )
    return (grad, small[0], small[1])


SENDS = 160
OTHERS = 72


def fits(mesh, args):
    rows, fin_width = args[0].shape
    width_s = args[1].shape[1]
    units = args[3].shape[1]
    group_count, fsdp_count = mesh.shape["group"], mesh.shape["fsdp"]
    devices = group_count * fsdp_count
    return (
        group_count == 2
        and fsdp_count == 16
        and units == devices * LANES
        and (rows // devices) % LANES == 0
        and (2 * width_s // fsdp_count) % LANES == 0
        and width_s % (2 * PAIRS * LANES) == 0
    )


def solution(mesh):
    in_specs = (
        P(("group", "fsdp"), None),
        P(("group", "fsdp"), None),
        P(("group", "fsdp")),
        P(None, ("group", "fsdp")),
        P(),
        P(),
        P(),
        P(),
        P(),
        P(),
    )
    out_specs = (P("fsdp", None), P(), P())

    def run(*args):
        body = shards_fused if fits(mesh, args) else shards
        return jax.shard_map(body, mesh=mesh, in_specs=in_specs, out_specs=out_specs, check_vma=False)(*args)

    return run
```

```python
import functools
import math

import jax
import jax.numpy as jnp
from jax import lax
from jax.experimental import pallas as pl
from jax.experimental.pallas import tpu as pltpu
from jax.sharding import PartitionSpec as P

epsilon = 1e-06


def shards(
    teacher_rows,
    student_rows,
    counts,
    teacher_weight,
    teacher_bias,
    teacher_gain,
    teacher_head,
    cross_weight,
    cross_bias,
    out_weight,
):
    row_count = teacher_rows.shape[0]
    width_s = cross_weight.shape[0]
    group_count = lax.axis_size("group")
    fsdp_count = lax.axis_size("fsdp")
    shard_count = group_count * fsdp_count
    loss_scale = math.sqrt(width_s / (row_count * shard_count))
    preact = jnp.dot(
        teacher_rows,
        lax.all_gather(teacher_weight, ("group", "fsdp"), axis=1, tiled=True),
        preferred_element_type=jnp.float32,
    )
    preact = preact + teacher_bias
    meansq = jnp.mean(preact * preact, axis=-1, keepdims=True)
    normed = preact * lax.rsqrt(meansq + epsilon) * teacher_gain
    teacher_logit = jnp.sum(jax.nn.silu(normed) * teacher_head, axis=-1)
    cross = jnp.dot(student_rows, cross_weight, preferred_element_type=jnp.float32) + cross_bias
    inputs_f = student_rows.astype(jnp.float32)
    mixed = inputs_f * cross + inputs_f
    student_logit = jnp.sum(mixed * out_weight, axis=-1)
    live_rows = (jnp.arange(row_count, dtype=jnp.int32) < counts[0]).astype(jnp.float32)
    error = (student_logit - teacher_logit) * live_rows * loss_scale
    dcross = error[:, None] * out_weight[None, :] * inputs_f
    dcross_half = dcross.astype(jnp.bfloat16)
    term_b = jnp.sum(dcross, axis=0)
    term_o = jnp.sum(error[:, None] * mixed, axis=0)
    term_w = lax.dot_general(
        student_rows, dcross_half, (((0,), (0,)), ((), ())), preferred_element_type=jnp.float32
    )
    totals = lax.psum((term_w, term_b, term_o), "group")
    grad_cross = lax.psum_scatter(totals[0], "fsdp", scatter_dimension=0, tiled=True)
    small_sums = lax.psum((totals[1], totals[2]), "fsdp")
    return (grad_cross, small_sums[0], small_sums[1])


MESH = pl.DeviceIdType.MESH
LANES = 128
PAIRS = 4
QUARTERS = 4
CODE_ROWS = 16
CODE_BITS = 15.0
CODE_MOST = 32767.0
PLAN = (
    (1, 0), (1, 1), (0, 0), (1, 2), (2, 0), (1, 3), (0, 1), (2, 1), (3, 0), (0, 2), (2, 2), (3, 1), (2, 3), (0, 3), (3, 2), (4, 0),
    (3, 3), (4, 1), (4, 2), (4, 3),
)


def fused(fsdp_count, rp, t_ref, s_ref, live_ref, w_ref, bias_ref, gain_ref, head_ref, cw_ref, cb_ref, ow_ref,
          out_ref, small_ref,
          wbuf, rows, xs, cw, pre, ssq, gains, heads, mixed, msg1, in1, msg2, in2, rr, er, xt, dbuf,
          ecol, tw, q1, r1, s1, q2, r2, tt, q3, r3, fin, r4, sb, rb, rz, lsem, ssem, rsem, wsem):
    g = lax.axis_index("group")
    f = lax.axis_index("fsdp")
    core = lax.rem(f, 2)
    x = lax.rem(lax.div(f, 2), 2)
    z = lax.div(f, 4)
    nz = fsdp_count // 4
    row_count, fin_width = t_ref.shape
    width_s = s_ref.shape[1]
    block = width_s // fsdp_count
    half_rows = block // 2
    rt = row_count // LANES
    units = bias_ref.shape[0] * LANES
    parts = 2 * PAIRS
    pw = width_s // parts

    def at(y_, z_, x_, c_):
        return (y_, (z_ * 2 + x_) * 2 + c_)

    partner = at(g, z, x, 1 - core)
    xn = at(g, z, 1 - x, core)
    yn = at(1 - g, z, x, core)
    barrier = pltpu.get_barrier_semaphore()
    peers = [partner, xn, yn] + [at(g, lax.rem(z + k, nz), x, core) for k in range(1, nz)]
    for peer in peers:
        pl.semaphore_signal(barrier, inc=1, device_id=peer, device_id_type=MESH)

    locals_ = []
    for i, (a, b) in enumerate([
        (s_ref, xs.at[pl.ds(0, row_count)]),
        (cw_ref, cw),
        (w_ref, wbuf.at[0]),
        (t_ref, rows.at[pl.ds(0, row_count)]),
    ]):
        cp = pltpu.make_async_copy(a, b, lsem.at[i])
        cp.start()
        locals_.append(cp)
    pl.semaphore_wait(barrier, len(peers))

    sends = []
    mid_sends = []
    end_sends = []
    waits = []
    turn = [0]

    def send(a, b, device, recv=None, only=None):
        i = turn[0]
        turn[0] += 1
        if recv is None:
            recv = rsem.at[len(waits)]
            waits.append(i)
        cp = pltpu.make_async_remote_copy(
            src_ref=a, dst_ref=b, send_sem=ssem.at[i], recv_sem=recv, device_id=device, device_id_type=MESH
        )
        cp.start()
        if only:
            (end_sends if only == 'end' else mid_sends).append(i)
        else:
            sends.append(cp)
        return cp

    half_z = lax.div(z, 2)
    is_mid = jnp.logical_or(z == 1, z == 2)
    is_end = jnp.logical_not(is_mid)
    plane = (z, z + 1 - 2 * lax.rem(z, 2), 2 - half_z, 3 - 3 * half_z)
    zpair = at(g, plane[1], x, core)
    zmid = at(g, nz - 1 - z, x, core)
    depth = fin_width // QUARTERS
    quarters = list(range(QUARTERS))
    first, last = quarters[:QUARTERS // 2], quarters[QUARTERS // 2:]

    def slot(dx, dy, n):
        return (dx * 2 + dy) * nz + n

    def piece(dx, dy, n, q):
        return wbuf.at[slot(dx, dy, n), pl.ds(q * depth, depth)]

    def arrival(dx, dy, n, q):
        return wsem.at[slot(dx, dy, n) * QUARTERS + q]

    def pass_on(src, dst, q, device, only=None):
        here = w_ref.at[pl.ds(q * depth, depth)] if src is None else piece(*src, q)
        send(here, piece(*dst, q), device, arrival(*dst, q), only)

    def landed(dx, dy, n, qs):
        for q in qs:
            pltpu.make_async_remote_copy(
                src_ref=piece(dx, dy, n, q), dst_ref=piece(dx, dy, n, q), send_sem=ssem.at[0],
                recv_sem=arrival(dx, dy, n, q), device_id=partner, device_id_type=MESH
            ).wait_recv()

    def sideways(src, n):
        for qx, qy in zip(last + first, quarters):
            pass_on(src, (1, 0, n), qx, xn)
            pass_on(src, (0, 1, n), qy, yn)

    for qx, q in zip(last + first, quarters):
        pass_on(None, (1, 0, 0), qx, xn)
        pass_on(None, (0, 1, 0), q, yn)
        pass_on(None, (0, 0, 1), q, zpair)

    @pl.when(is_mid)
    def _():
        for q in quarters:
            pass_on(None, (0, 0, 2), q, zmid, 'mid')

    rows_in = send(t_ref, rows.at[pl.ds(row_count, row_count)], partner)
    xs_in = send(s_ref, xs.at[pl.ds(row_count, row_count)], partner)

    def diagonal(n):
        for qx, qy in zip(first, last):
            landed(0, 1, n, [qx])
            pass_on((0, 1, n), (1, 1, n), qx, xn)
            landed(1, 0, n, [qy])
            pass_on((1, 0, n), (1, 1, n), qy, yn)

    def rest(n):
        landed(0, 1, n, last)
        landed(1, 0, n, first)

    eye = lax.broadcasted_iota(jnp.int32, (LANES, LANES), 0) == lax.broadcasted_iota(jnp.int32, (LANES, LANES), 1)

    def to_row(col):
        return jnp.sum(jnp.where(eye, col, 0.0), axis=0, keepdims=True)

    def to_col(row):
        return jnp.sum(jnp.where(eye, row, 0.0), axis=1, keepdims=True)

    def tile(t):
        return pl.ds(pl.multiple_of(t * LANES, LANES), LANES)

    ssq[...] = jnp.zeros_like(ssq)
    for ref in (msg1, msg2, er, rr):
        ref[...] = jnp.zeros_like(ref)
    msg1[pl.ds(3 * rp, rt), :] = live_ref[...]

    locals_[0].wait()
    locals_[1].wait()
    ow = ow_ref[...]

    def student(t, carry):
        xt_ = xs[tile(t), :]
        cross = jnp.dot(xt_, cw[...], preferred_element_type=jnp.float32) + cb_ref[...]
        xf = xt_.astype(jnp.float32)
        m = xf * cross + xf
        mixed[tile(t), :] = m
        msg1[pl.ds(2 * rp + t, 1), :] = to_row(jnp.sum(m * ow, axis=1, keepdims=True))
        return carry

    lax.fori_loop(0, rt, student, 0)
    locals_[2].wait()
    locals_[3].wait()

    mt = row_count

    def project(dx, dy, n):
        s = slot(dx, dy, n)
        y_ = g if dy == 0 else 1 - g
        x_ = x if dx == 0 else 1 - x
        index = y_ * fsdp_count + (plane[n] * 2 + x_) * 2 + core
        gains[pl.ds(s, 1), :] = gain_ref[index] * 0.5
        heads[pl.ds(s, 1), :] = head_ref[index]
        bias = bias_ref[index]

        def step(t, carry):
            ds = pl.ds(pl.multiple_of(t * mt, mt), mt)
            p = jnp.dot(rows[ds, :], wbuf[s], preferred_element_type=jnp.float32) + bias
            pre[s, ds, :] = p
            ssq[ds, :] += p * p
            return carry

        lax.fori_loop(0, 2 * row_count // mt, step, 0)

    order = [q for pair in zip(first, last) for q in pair]

    for i, (qx, qy) in enumerate(zip(first, last)):
        landed(0, 1, 0, [qx])
        pass_on((0, 1, 0), (1, 1, 0), qx, xn)
        landed(1, 0, 0, [qy])
        pass_on((1, 0, 0), (1, 1, 0), qy, yn)

        @pl.when(is_mid)
        def _(i=i):
            for q in quarters[2 * i:2 * i + 2]:
                landed(0, 0, 2, [q])
                pass_on((0, 0, 2), (0, 0, 2), q, zpair, 'mid')
                landed(0, 0, 1, [q])
                pass_on((0, 0, 1), (0, 0, 3), q, zmid, 'mid')

    rows_in.wait_recv()
    project(0, 0, 0)

    @pl.when(is_end)
    def _():
        landed(0, 0, 1, quarters)

    sideways((0, 0, 1), 1)
    rest(0)
    project(1, 0, 0)

    def far(q):
        landed(0, 0, 3, [q])
        pass_on((0, 0, 3), (0, 0, 3), q, zpair, 'mid')

    @pl.when(is_mid)
    def _():
        far(0)

    project(0, 1, 0)
    for i, q in enumerate(order):
        landed(1, 1, 0, [q])

        @pl.when(is_end)
        def _(q=q):
            pass_on((1, 1, 0), (1, 1, 1), q, zpair, 'end')

        @pl.when(is_mid)
        def _(q=q, i=i):
            pass_on((1, 1, 0), (1, 1, 2), q, zmid, 'mid')
            if i == 1:
                far(1)

    project(0, 0, 1)
    xs_in.wait_recv()
    pick = (
        lax.broadcasted_iota(jnp.int32, (block, 2 * block), 1)
        == lax.broadcasted_iota(jnp.int32, (block, 2 * block), 0) + core * block
    )
    pick = jnp.where(pick, 1.0, 0.0).astype(jnp.bfloat16)
    for j in range(fsdp_count // 2):
        xt[pl.ds(j * block, block), :] = lax.dot_general(
            pick, xs[:, pl.ds(j * 2 * block, 2 * block)], (((1,), (1,)), ((), ())), preferred_element_type=jnp.float32
        ).astype(jnp.bfloat16)

    @pl.when(is_mid)
    def _():
        for q in quarters[2:]:
            far(q)
        for q in order:
            pass_on((1, 1, 0), (1, 1, 1), q, zpair, 'mid')

    @pl.when(is_end)
    def _():
        landed(0, 0, 2, quarters)

    sideways((0, 0, 2), 2)
    project(1, 1, 0)
    project(0, 0, 2)
    landed(1, 0, 1, quarters)
    project(1, 0, 1)
    landed(0, 1, 1, quarters)

    @pl.when(is_end)
    def _():
        landed(0, 0, 3, quarters)

    sideways((0, 0, 3), 3)
    project(0, 1, 1)

    @pl.when(is_mid)
    def _():
        for q in order:
            landed(1, 1, 2, [q])
            pass_on((1, 1, 2), (1, 1, 2), q, zpair, 'mid')

    project(0, 0, 3)
    for at_ in ((1, 0, 2), (0, 1, 2)):
        landed(*at_, quarters)
        project(*at_)
    diagonal(3)
    landed(1, 1, 1, quarters)
    project(1, 1, 1)
    rest(3)
    project(1, 0, 3)
    project(0, 1, 3)

    @pl.when(is_end)
    def _():
        landed(1, 1, 2, quarters)

    project(1, 1, 2)
    landed(1, 1, 3, quarters)
    project(1, 1, 3)

    for h in range(2):
        def squares(t, carry, h=h):
            col = jnp.sum(ssq[tile(h * rt + t), :], axis=1, keepdims=True)
            msg1[pl.ds(h * rp + t, 1), :] = to_row(col)
            return carry

        lax.fori_loop(0, rt, squares, 0)
    m1 = send(msg1, in1, partner)
    m1.wait_recv()
    for h in range(2):
        total = msg1[pl.ds(h * rp, rp), :] + in1[pl.ds((1 - h) * rp, rp), :]
        rr[pl.ds(h * rp, rp), :] = lax.rsqrt(total * (1.0 / units) + epsilon)

    for h in range(2):
        def logits(t, carry, h=h):
            r = to_col(rr[pl.ds(h * rp + t, 1), :])
            acc = jnp.zeros((LANES, LANES), jnp.float32)
            for s in range(4 * nz):
                v = pre[s, tile(h * rt + t), :] * r * gains[pl.ds(s, 1), :]
                acc += (v * jnp.tanh(v) + v) * heads[pl.ds(s, 1), :]
            msg2[pl.ds(h * rp + t, 1), :] = to_row(jnp.sum(acc, axis=1, keepdims=True))
            return carry

        lax.fori_loop(0, rt, logits, 0)
    m2 = send(msg2, in2, partner)
    m2.wait_recv()
    for h, src in ((0, msg1), (1, in1)):
        teacher = msg2[pl.ds(h * rp, rp), :] + in2[pl.ds((1 - h) * rp, rp), :]
        er[pl.ds(h * rp, rp), :] = (src[pl.ds(2 * rp, rp), :] - teacher) * src[pl.ds(3 * rp, rp), :]

    def spread(t, carry):
        ecol[tile(t), :] = jnp.broadcast_to(to_col(er[pl.ds(t, 1), :]), (LANES, LANES))
        ecol[tile(rt + t), :] = jnp.broadcast_to(to_col(er[pl.ds(rp + t, 1), :]), (LANES, LANES))
        return carry

    lax.fori_loop(0, rt, spread, 0)
    sb[...] = jnp.zeros_like(sb)

    def scale_cross(p):
        cols = pl.ds(p * pw, pw)
        owp = ow_ref[:, cols]

        def cross_tile(t, carry):
            d = ecol[tile(t), :] * owp * xs[tile(t), cols].astype(jnp.float32)
            dbuf[tile(t), cols] = d.astype(jnp.bfloat16)
            return carry

        lax.fori_loop(0, 2 * rt, cross_tile, 0)

    def small_terms():
        def one(t, carry):
            for p in range(parts):
                cols = pl.ds(p * pw, pw)
                e = ecol[tile(t), :]
                d = e * ow_ref[:, cols] * xs[tile(t), cols].astype(jnp.float32)
                sb[0, pl.ds(0, 1), cols] += jnp.sum(d, axis=0, keepdims=True)
                sb[0, pl.ds(1, 1), cols] += jnp.sum(e * mixed[tile(t), cols], axis=0, keepdims=True)
            return carry

        lax.fori_loop(0, rt, one, 0)

    exp_row = lax.broadcasted_iota(jnp.int32, (CODE_ROWS, pw), 0)

    def encode(blocks, msg):
        exps = jnp.zeros((CODE_ROWS, pw), jnp.float32)
        for i, v in enumerate(blocks):
            most = jnp.max(jnp.abs(v), axis=0, keepdims=True)
            e = jnp.ceil(jnp.log2(jnp.maximum(most, 1e-30)))
            exps = jnp.where(exp_row == i, e, exps)
            q = jnp.clip(jnp.round(v * jnp.exp2(CODE_BITS - e)), -CODE_MOST, CODE_MOST)
            msg[pl.ds(i * half_rows, half_rows), :] = q.astype(jnp.int32).astype(jnp.int16)
        msg[pl.ds(len(blocks) * half_rows, CODE_ROWS), :] = exps.astype(jnp.int32).astype(jnp.int16)

    def decode(msg, n):
        exps = msg[pl.ds(n * half_rows, CODE_ROWS), :].astype(jnp.int32).astype(jnp.float32)
        step = jnp.exp2(exps - CODE_BITS)
        out = []
        for i in range(n):
            q = msg[pl.ds(i * half_rows, half_rows), :].astype(jnp.int32).astype(jnp.float32)
            out.append(q * step[i:i + 1, :])
        return out

    def way(p):
        return (g, x, yn, xn) if p % 2 == 0 else (x, g, xn, yn)

    h1, h2, h3, h4 = {}, {}, {}, {}

    def stage1(q):
        for p in (2 * q, 2 * q + 1):
            scale_cross(p)
            val = jnp.dot(xt[...], dbuf[:, pl.ds(p * pw, pw)], preferred_element_type=jnp.float32)
            for z_ in range(nz):
                for x_ in range(2):
                    for y_ in range(2):
                        first, second = (y_, x_) if p % 2 == 0 else (x_, y_)
                        offset = ((z_ * 2 + x_) * 2 + y_) * half_rows
                        tw[p, first, second, z_] = val[offset:offset + half_rows, :]
            first, second, n1, n2 = way(p)
            encode([tw[p, 1 - first, s_, z_] for s_ in range(2) for z_ in range(nz)], q1.at[p])
            h1[p] = send(q1.at[p], r1.at[p], n1)

    def stage2(q):
        for p in (2 * q, 2 * q + 1):
            first, second, n1, n2 = way(p)
            h1[p].wait_recv()
            for i, v in enumerate(decode(r1.at[p], 2 * nz)):
                s1[p, i // nz, i % nz] = tw[p, first, i // nz, i % nz] + v
            encode([s1[p, 1 - second, z_] for z_ in range(nz)], q2.at[p])
            h2[p] = send(q2.at[p], r2.at[p], n2)

    def stage3(q):
        for p in (2 * q, 2 * q + 1):
            first, second, n1, n2 = way(p)
            h2[p].wait_recv()
            for z_, v in enumerate(decode(r2.at[p], nz)):
                tt[p, z_] = s1[p, second, z_] + v
        for z_ in range(nz):
            encode([tt[2 * q, z_], tt[2 * q + 1, z_]], q3.at[q, z_])
        h3[q] = []
        for k in range(1, nz):
            to = lax.rem(z + k, nz)
            h3[q].append(send(q3.at[q, to], r3.at[q, k - 1], at(g, to, x, core)))

    def stage4(q):
        totals = [tt[2 * q, z], tt[2 * q + 1, z]]
        for k in range(nz - 1):
            h3[q][k].wait_recv()
            totals = [t + v for t, v in zip(totals, decode(r3.at[q, k], 2))]
        for i, total in enumerate(totals):
            p = 2 * q + i
            fin[q, :, pl.ds(i * pw, pw)] = total
            out_ref[pl.ds(pl.multiple_of(g * half_rows, half_rows), half_rows), pl.ds(p * pw, pw)] = total
        h4[q] = send(fin.at[q], r4.at[q], yn)

    cz = []

    def small(n):
        if n == 0:
            cz.pop().wait_recv()
            sb[1] = sb[0] + rb[0]
            cz.append(send(sb.at[1], rb.at[1], xn))
        elif n == 1:
            cz.pop().wait_recv()
            sb[2] = sb[1] + rb[1]
            cz.append(send(sb.at[2], rb.at[2], yn))
        elif n == 2:
            cz.pop().wait_recv()
            sb[3] = sb[2] + rb[2]
            rz[z] = sb[3]
            for k in range(1, nz):
                to = lax.rem(z + k, nz)
                cz.append(send(sb.at[3], rz.at[z], at(g, to, x, core)))

    for stage, q in PLAN:
        if stage == 0:
            if q == 0:
                small_terms()
                cz.append(send(sb.at[0], rb.at[0], partner))
            else:
                small(q - 1)
        else:
            (stage1, stage2, stage3, stage4)[stage - 1](q)
    for cp in cz:
        cp.wait_recv()
    total = rz[0]
    for k in range(1, nz):
        total = total + rz[k]
    small_ref[...] = total
    for q in range(PAIRS):
        h4[q].wait_recv()
        out_ref[pl.ds(pl.multiple_of((1 - g) * half_rows, half_rows), half_rows), pl.ds(2 * q * pw, 2 * pw)] = r4[q]
    for cp in sends:
        cp.wait_send()

    for kind, some in ((is_mid, mid_sends), (is_end, end_sends)):
        @pl.when(kind)
        def _(some=some):
            for i in some:
                pltpu.make_async_remote_copy(
                    src_ref=piece(0, 0, 0, 0), dst_ref=piece(0, 0, 0, 0), send_sem=ssem.at[i], recv_sem=wsem.at[0],
                    device_id=partner, device_id_type=MESH
                ).wait_send()


def shards_fused(
    teacher_rows,
    student_rows,
    counts,
    teacher_weight,
    teacher_bias,
    teacher_gain,
    teacher_head,
    cross_weight,
    cross_bias,
    out_weight,
):
    row_count, fin_width = teacher_rows.shape
    width_s = cross_weight.shape[0]
    group_count = lax.axis_size("group")
    fsdp_count = lax.axis_size("fsdp")
    loss_scale = math.sqrt(width_s / (row_count * group_count * fsdp_count))
    live = (jnp.arange(row_count, dtype=jnp.int32) < counts[0]).astype(jnp.float32) * loss_scale
    rt = row_count // LANES
    rp = -(-rt // 8) * 8
    nz = fsdp_count // 4
    block = width_s // fsdp_count
    half_rows = block // 2
    parts = 2 * PAIRS
    pw = width_s // parts
    slots = 4 * nz
    f32, bf16, i16 = jnp.float32, jnp.bfloat16, jnp.int16
    vm = pltpu.VMEM
    split = lambda v: v.reshape(-1, 1, LANES)
    anyspec = pl.BlockSpec(memory_space=pl.ANY)
    vspec = pl.BlockSpec(memory_space=pltpu.VMEM)
    grad, small = pl.pallas_call(
        functools.partial(fused, fsdp_count, rp),
        out_shape=(jax.ShapeDtypeStruct((block, width_s), f32), jax.ShapeDtypeStruct((8, width_s), f32)),
        in_specs=[anyspec, anyspec, vspec, anyspec, vspec, vspec, vspec, anyspec, vspec, vspec],
        out_specs=(vspec, vspec),
        scratch_shapes=[
            vm((slots, fin_width, LANES), bf16),
            vm((2 * row_count, fin_width), bf16),
            vm((2 * row_count, width_s), bf16),
            vm((width_s, width_s), bf16),
            vm((slots, 2 * row_count, LANES), f32),
            vm((2 * row_count, LANES), f32),
            vm((slots, LANES), f32),
            vm((slots, LANES), f32),
            vm((row_count, width_s), f32),
            vm((4 * rp, LANES), f32),
            vm((4 * rp, LANES), f32),
            vm((2 * rp, LANES), f32),
            vm((2 * rp, LANES), f32),
            vm((2 * rp, LANES), f32),
            vm((2 * rp, LANES), f32),
            vm((width_s // 2, 2 * row_count), bf16),
            vm((2 * row_count, width_s), bf16),
            vm((2 * row_count, LANES), f32),
            vm((parts, 2, 2, nz, half_rows, pw), f32),
            vm((parts, 2 * nz * half_rows + CODE_ROWS, pw), i16),
            vm((parts, 2 * nz * half_rows + CODE_ROWS, pw), i16),
            vm((parts, 2, nz, half_rows, pw), f32),
            vm((parts, nz * half_rows + CODE_ROWS, pw), i16),
            vm((parts, nz * half_rows + CODE_ROWS, pw), i16),
            vm((parts, nz, half_rows, pw), f32),
            vm((PAIRS, nz, 2 * half_rows + CODE_ROWS, pw), i16),
            vm((PAIRS, nz - 1, 2 * half_rows + CODE_ROWS, pw), i16),
            vm((PAIRS, half_rows, 2 * pw), f32),
            vm((PAIRS, half_rows, 2 * pw), f32),
            vm((4, 8, width_s), f32),
            vm((3, 8, width_s), f32),
            vm((nz, 8, width_s), f32),
            pltpu.SemaphoreType.DMA((4,)),
            pltpu.SemaphoreType.DMA((SENDS,)),
            pltpu.SemaphoreType.DMA((OTHERS,)),
            pltpu.SemaphoreType.DMA((slots * QUARTERS,)),
        ],
        compiler_params=pltpu.CompilerParams(
            collective_id=0, has_side_effects=True, vmem_limit_bytes=60 * 1024 * 1024
        ),
    )(
        teacher_rows, student_rows, live.reshape(rt, LANES), teacher_weight, split(teacher_bias), split(teacher_gain),
        split(teacher_head), cross_weight, cross_bias[None, :], out_weight[None, :],
    )
    return (grad, small[0], small[1])


SENDS = 160
OTHERS = 72


def fits(mesh, args):
    rows, fin_width = args[0].shape
    width_s = args[1].shape[1]
    units = args[3].shape[1]
    group_count, fsdp_count = mesh.shape["group"], mesh.shape["fsdp"]
    devices = group_count * fsdp_count
    return (
        group_count == 2
        and fsdp_count == 16
        and units == devices * LANES
        and (rows // devices) % LANES == 0
        and (2 * width_s // fsdp_count) % LANES == 0
        and width_s == 2 * PAIRS * LANES
    )


def solution(mesh):
    in_specs = (
        P(("group", "fsdp"), None),
        P(("group", "fsdp"), None),
        P(("group", "fsdp")),
        P(None, ("group", "fsdp")),
        P(),
        P(),
        P(),
        P(),
        P(),
        P(),
    )
    out_specs = (P("fsdp", None), P(), P())

    def run(*args):
        body = shards_fused if fits(mesh, args) else shards
        return jax.shard_map(body, mesh=mesh, in_specs=in_specs, out_specs=out_specs, check_vma=False)(*args)

    return run
```

```python
import functools
import math

import jax
import jax.numpy as jnp
from jax import lax
from jax.experimental import pallas as pl
from jax.experimental.pallas import tpu as pltpu
from jax.sharding import PartitionSpec as P

epsilon = 1e-06


def shards(
    teacher_rows,
    student_rows,
    counts,
    teacher_weight,
    teacher_bias,
    teacher_gain,
    teacher_head,
    cross_weight,
    cross_bias,
    out_weight,
):
    row_count = teacher_rows.shape[0]
    width_s = cross_weight.shape[0]
    group_count = lax.axis_size("group")
    fsdp_count = lax.axis_size("fsdp")
    shard_count = group_count * fsdp_count
    loss_scale = math.sqrt(width_s / (row_count * shard_count))
    preact = jnp.dot(
        teacher_rows,
        lax.all_gather(teacher_weight, ("group", "fsdp"), axis=1, tiled=True),
        preferred_element_type=jnp.float32,
    )
    preact = preact + teacher_bias
    meansq = jnp.mean(preact * preact, axis=-1, keepdims=True)
    normed = preact * lax.rsqrt(meansq + epsilon) * teacher_gain
    teacher_logit = jnp.sum(jax.nn.silu(normed) * teacher_head, axis=-1)
    cross = jnp.dot(student_rows, cross_weight, preferred_element_type=jnp.float32) + cross_bias
    inputs_f = student_rows.astype(jnp.float32)
    mixed = inputs_f * cross + inputs_f
    student_logit = jnp.sum(mixed * out_weight, axis=-1)
    live_rows = (jnp.arange(row_count, dtype=jnp.int32) < counts[0]).astype(jnp.float32)
    error = (student_logit - teacher_logit) * live_rows * loss_scale
    dcross = error[:, None] * out_weight[None, :] * inputs_f
    dcross_half = dcross.astype(jnp.bfloat16)
    term_b = jnp.sum(dcross, axis=0)
    term_o = jnp.sum(error[:, None] * mixed, axis=0)
    term_w = lax.dot_general(
        student_rows, dcross_half, (((0,), (0,)), ((), ())), preferred_element_type=jnp.float32
    )
    totals = lax.psum((term_w, term_b, term_o), "group")
    grad_cross = lax.psum_scatter(totals[0], "fsdp", scatter_dimension=0, tiled=True)
    small_sums = lax.psum((totals[1], totals[2]), "fsdp")
    return (grad_cross, small_sums[0], small_sums[1])


MESH = pl.DeviceIdType.MESH
LANES = 128
PAIRS = 4
QUARTERS = 4
CODE_ROWS = 16
CODE_BITS = 15.0
CODE_MOST = 32767.0
PLAN = (
    (1, 0), (1, 1), (0, 0), (1, 2), (2, 0), (1, 3), (0, 1), (2, 1), (3, 0), (0, 2), (2, 2), (3, 1), (2, 3), (0, 3), (3, 2), (4, 0),
    (3, 3), (4, 1), (4, 2), (4, 3),
)


def fused(fsdp_count, rp, loss_scale, t_ref, s_ref, count_ref, w_ref, bias_ref, gain_ref, head_ref, cw_ref, cb_ref, ow_ref,
          out_ref, small_ref,
          wbuf, rows, xs, cw, pre, ssq, heads, mixed, msg1, in1, msg2, in2, rr, er, xt, dbuf,
          ecol, tw, q1, r1, s1, q2, r2, tt, q3, r3, fin, r4, sb, rb, rz, lsem, ssem, rsem, wsem):
    g = lax.axis_index("group")
    f = lax.axis_index("fsdp")
    core = lax.rem(f, 2)
    x = lax.rem(lax.div(f, 2), 2)
    z = lax.div(f, 4)
    nz = fsdp_count // 4
    row_count, fin_width = t_ref.shape
    width_s = s_ref.shape[1]
    block = width_s // fsdp_count
    half_rows = block // 2
    rt = row_count // LANES
    units = bias_ref.shape[0] * LANES
    parts = 2 * PAIRS
    pw = width_s // parts

    def at(y_, z_, x_, c_):
        return (y_, (z_ * 2 + x_) * 2 + c_)

    partner = at(g, z, x, 1 - core)
    xn = at(g, z, 1 - x, core)
    yn = at(1 - g, z, x, core)
    barrier = pltpu.get_barrier_semaphore()
    peers = [partner, xn, yn] + [at(g, lax.rem(z + k, nz), x, core) for k in range(1, nz)]
    for peer in peers:
        pl.semaphore_signal(barrier, inc=1, device_id=peer, device_id_type=MESH)

    locals_ = []
    for i, (a, b) in enumerate([
        (s_ref, xs.at[pl.ds(0, row_count)]),
        (cw_ref, cw),
        (w_ref, wbuf.at[0]),
        (t_ref, rows.at[pl.ds(0, row_count)]),
    ]):
        cp = pltpu.make_async_copy(a, b, lsem.at[i])
        cp.start()
        locals_.append(cp)
    pl.semaphore_wait(barrier, len(peers))

    sends = []
    mid_sends = []
    end_sends = []
    waits = []
    turn = [0]

    def send(a, b, device, recv=None, only=None):
        i = turn[0]
        turn[0] += 1
        if recv is None:
            recv = rsem.at[len(waits)]
            waits.append(i)
        cp = pltpu.make_async_remote_copy(
            src_ref=a, dst_ref=b, send_sem=ssem.at[i], recv_sem=recv, device_id=device, device_id_type=MESH
        )
        cp.start()
        if only:
            (end_sends if only == 'end' else mid_sends).append(i)
        else:
            sends.append(cp)
        return cp

    half_z = lax.div(z, 2)
    is_mid = jnp.logical_or(z == 1, z == 2)
    is_end = jnp.logical_not(is_mid)
    plane = (z, z + 1 - 2 * lax.rem(z, 2), 2 - half_z, 3 - 3 * half_z)
    zpair = at(g, plane[1], x, core)
    zmid = at(g, nz - 1 - z, x, core)
    depth = fin_width // QUARTERS
    quarters = list(range(QUARTERS))
    first, last = quarters[:QUARTERS // 2], quarters[QUARTERS // 2:]

    def slot(dx, dy, n):
        return (dx * 2 + dy) * nz + n

    def piece(dx, dy, n, q):
        return wbuf.at[slot(dx, dy, n), pl.ds(q * depth, depth)]

    def arrival(dx, dy, n, q):
        return wsem.at[slot(dx, dy, n) * QUARTERS + q]

    def pass_on(src, dst, q, device, only=None):
        here = w_ref.at[pl.ds(q * depth, depth)] if src is None else piece(*src, q)
        send(here, piece(*dst, q), device, arrival(*dst, q), only)

    def landed(dx, dy, n, qs):
        for q in qs:
            pltpu.make_async_remote_copy(
                src_ref=piece(dx, dy, n, q), dst_ref=piece(dx, dy, n, q), send_sem=ssem.at[0],
                recv_sem=arrival(dx, dy, n, q), device_id=partner, device_id_type=MESH
            ).wait_recv()

    def sideways(src, n):
        for qx, qy in zip(last + first, quarters):
            pass_on(src, (1, 0, n), qx, xn)
            pass_on(src, (0, 1, n), qy, yn)

    for qx, q in zip(last + first, quarters):
        pass_on(None, (1, 0, 0), qx, xn)
        pass_on(None, (0, 1, 0), q, yn)
        pass_on(None, (0, 0, 1), q, zpair)

    @pl.when(is_mid)
    def _():
        for q in quarters:
            pass_on(None, (0, 0, 2), q, zmid, 'mid')

    rows_in = send(t_ref, rows.at[pl.ds(row_count, row_count)], partner)
    xs_in = send(s_ref, xs.at[pl.ds(row_count, row_count)], partner)

    def diagonal(n):
        for qx, qy in zip(first, last):
            landed(0, 1, n, [qx])
            pass_on((0, 1, n), (1, 1, n), qx, xn)
            landed(1, 0, n, [qy])
            pass_on((1, 0, n), (1, 1, n), qy, yn)

    def rest(n):
        landed(0, 1, n, last)
        landed(1, 0, n, first)

    eye = lax.broadcasted_iota(jnp.int32, (LANES, LANES), 0) == lax.broadcasted_iota(jnp.int32, (LANES, LANES), 1)

    def to_row(col):
        return jnp.sum(jnp.where(eye, col, 0.0), axis=0, keepdims=True)

    def to_col(row):
        return jnp.sum(jnp.where(eye, row, 0.0), axis=1, keepdims=True)

    def tile(t):
        return pl.ds(pl.multiple_of(t * LANES, LANES), LANES)

    ssq[...] = jnp.zeros_like(ssq)
    for ref in (msg1, msg2, er, rr):
        ref[...] = jnp.zeros_like(ref)
    row = lax.broadcasted_iota(jnp.int32, (rt, LANES), 0) * LANES + lax.broadcasted_iota(jnp.int32, (rt, LANES), 1)
    msg1[pl.ds(3 * rp, rt), :] = jnp.where(row < count_ref[0], loss_scale, 0.0)

    locals_[0].wait()
    locals_[1].wait()
    ow = ow_ref[...]

    def student(t, carry):
        xt_ = xs[tile(t), :]
        cross = jnp.dot(xt_, cw[...], preferred_element_type=jnp.float32) + cb_ref[...]
        xf = xt_.astype(jnp.float32)
        m = xf * cross + xf
        mixed[tile(t), :] = m
        msg1[pl.ds(2 * rp + t, 1), :] = to_row(jnp.sum(m * ow, axis=1, keepdims=True))
        return carry

    lax.fori_loop(0, rt, student, 0)
    locals_[2].wait()
    locals_[3].wait()

    mt = row_count

    def column_block(dx, dy, n):
        y_ = g if dy == 0 else 1 - g
        x_ = x if dx == 0 else 1 - x
        return y_ * fsdp_count + (plane[n] * 2 + x_) * 2 + core

    def project(*blocks):
        found = []
        for b_ in blocks:
            index = column_block(*b_)
            heads[pl.ds(slot(*b_), 1), :] = head_ref[index]
            found.append((slot(*b_), gain_ref[index] * 0.5, bias_ref[index]))

        def step(t, carry):
            ds = pl.ds(pl.multiple_of(t * mt, mt), mt)
            w = jnp.concatenate([wbuf[s] for s, _, _ in found], axis=1) if len(found) > 1 else wbuf[found[0][0]]
            both = jnp.dot(rows[ds, :], w, preferred_element_type=jnp.float32)
            for i, (s, gain, bias) in enumerate(found):
                p = both[:, i * LANES:(i + 1) * LANES] + bias
                pre[s, ds, :] = p * gain
                ssq[ds, :] += p * p
            return carry

        lax.fori_loop(0, 2 * row_count // mt, step, 0)

    order = [q for pair in zip(first, last) for q in pair]

    for i, (qx, qy) in enumerate(zip(first, last)):
        landed(0, 1, 0, [qx])
        pass_on((0, 1, 0), (1, 1, 0), qx, xn)
        landed(1, 0, 0, [qy])
        pass_on((1, 0, 0), (1, 1, 0), qy, yn)

        @pl.when(is_mid)
        def _(i=i):
            for q in quarters[2 * i:2 * i + 2]:
                landed(0, 0, 2, [q])
                pass_on((0, 0, 2), (0, 0, 2), q, zpair, 'mid')
                landed(0, 0, 1, [q])
                pass_on((0, 0, 1), (0, 0, 3), q, zmid, 'mid')

    rows_in.wait_recv()
    project((0, 0, 0))

    @pl.when(is_end)
    def _():
        landed(0, 0, 1, quarters)

    sideways((0, 0, 1), 1)
    rest(0)
    project((1, 0, 0))

    def far(q):
        landed(0, 0, 3, [q])
        pass_on((0, 0, 3), (0, 0, 3), q, zpair, 'mid')

    @pl.when(is_mid)
    def _():
        far(0)

    project((0, 1, 0))
    for i, q in enumerate(order):
        landed(1, 1, 0, [q])

        @pl.when(is_end)
        def _(q=q):
            pass_on((1, 1, 0), (1, 1, 1), q, zpair, 'end')

        @pl.when(is_mid)
        def _(q=q, i=i):
            pass_on((1, 1, 0), (1, 1, 2), q, zmid, 'mid')
            if i == 1:
                far(1)

    project((0, 0, 1))
    xs_in.wait_recv()
    pick = (
        lax.broadcasted_iota(jnp.int32, (block, 2 * block), 1)
        == lax.broadcasted_iota(jnp.int32, (block, 2 * block), 0) + core * block
    )
    pick = jnp.where(pick, 1.0, 0.0).astype(jnp.bfloat16)
    for j in range(fsdp_count // 2):
        turned = lax.dot_general(
            pick, xs[:, pl.ds(j * 2 * block, 2 * block)], (((1,), (1,)), ((), ())), preferred_element_type=jnp.float32
        ).astype(jnp.bfloat16)
        far_x = lax.rem(x + j % 2, 2)
        for y_ in range(2):
            to = ((lax.rem(g + y_, 2) * 2 + far_x) * nz + j // 2) * half_rows
            xt[pl.ds(pl.multiple_of(to, half_rows), half_rows), :] = turned[y_ * half_rows:(y_ + 1) * half_rows, :]

    @pl.when(is_mid)
    def _():
        for q in quarters[2:]:
            far(q)
        for q in order:
            pass_on((1, 1, 0), (1, 1, 1), q, zpair, 'mid')

    @pl.when(is_end)
    def _():
        landed(0, 0, 2, quarters)

    sideways((0, 0, 2), 2)
    project((1, 1, 0))
    project((0, 0, 2))
    landed(1, 0, 1, quarters)
    project((1, 0, 1))
    landed(0, 1, 1, quarters)

    @pl.when(is_end)
    def _():
        landed(0, 0, 3, quarters)

    sideways((0, 0, 3), 3)
    project((0, 1, 1))

    @pl.when(is_mid)
    def _():
        for q in order:
            landed(1, 1, 2, [q])
            pass_on((1, 1, 2), (1, 1, 2), q, zpair, 'mid')

    project((0, 0, 3))
    for at_ in ((1, 0, 2), (0, 1, 2)):
        landed(*at_, quarters)
        project(at_)
    diagonal(3)
    landed(1, 1, 1, quarters)
    project((1, 1, 1))
    rest(3)
    project((1, 0, 3))
    project((0, 1, 3))

    @pl.when(is_end)
    def _():
        landed(1, 1, 2, quarters)

    landed(1, 1, 3, quarters)
    project((1, 1, 2), (1, 1, 3))

    for h in range(2):
        def squares(t, carry, h=h):
            col = jnp.sum(ssq[tile(h * rt + t), :], axis=1, keepdims=True)
            msg1[pl.ds(h * rp + t, 1), :] = to_row(col)
            return carry

        lax.fori_loop(0, rt, squares, 0)
    m1 = send(msg1, in1, partner)
    m1.wait_recv()
    for h in range(2):
        total = msg1[pl.ds(h * rp, rp), :] + in1[pl.ds((1 - h) * rp, rp), :]
        rr[pl.ds(h * rp, rp), :] = lax.rsqrt(total * (1.0 / units) + epsilon)

    for h in range(2):
        def logits(t, carry, h=h):
            r = to_col(rr[pl.ds(h * rp + t, 1), :])
            acc = jnp.zeros((LANES, LANES), jnp.float32)
            for s in range(4 * nz):
                v = pre[s, tile(h * rt + t), :] * r
                acc += (v * jnp.tanh(v) + v) * heads[pl.ds(s, 1), :]
            msg2[pl.ds(h * rp + t, 1), :] = to_row(jnp.sum(acc, axis=1, keepdims=True))
            return carry

        lax.fori_loop(0, rt, logits, 0)
    m2 = send(msg2, in2, partner)
    m2.wait_recv()
    for h, src in ((0, msg1), (1, in1)):
        teacher = msg2[pl.ds(h * rp, rp), :] + in2[pl.ds((1 - h) * rp, rp), :]
        er[pl.ds(h * rp, rp), :] = (src[pl.ds(2 * rp, rp), :] - teacher) * src[pl.ds(3 * rp, rp), :]

    def spread(t, carry):
        ecol[tile(t), :] = jnp.broadcast_to(to_col(er[pl.ds(t, 1), :]), (LANES, LANES))
        ecol[tile(rt + t), :] = jnp.broadcast_to(to_col(er[pl.ds(rp + t, 1), :]), (LANES, LANES))
        return carry

    lax.fori_loop(0, rt, spread, 0)
    sb[...] = jnp.zeros_like(sb)

    def scale_cross(q):
        cols = pl.ds(2 * q * pw, 2 * pw)
        owp = ow_ref[:, cols]

        def cross_tile(t, carry):
            e = ecol[tile(t), :]
            d = jnp.concatenate([e, e], axis=1) * owp * xs[tile(t), cols].astype(jnp.float32)
            dbuf[tile(t), cols] = d.astype(jnp.bfloat16)
            return carry

        lax.fori_loop(0, 2 * rt, cross_tile, 0, unroll=2)

    def small_terms():
        def one(t, carry):
            for p in range(parts):
                cols = pl.ds(p * pw, pw)
                e = ecol[tile(t), :]
                d = e * ow_ref[:, cols] * xs[tile(t), cols].astype(jnp.float32)
                sb[0, pl.ds(0, 1), cols] += jnp.sum(d, axis=0, keepdims=True)
                sb[0, pl.ds(1, 1), cols] += jnp.sum(e * mixed[tile(t), cols], axis=0, keepdims=True)
            return carry

        lax.fori_loop(0, rt, one, 0)

    exp_row = lax.broadcasted_iota(jnp.int32, (CODE_ROWS, pw), 0)

    def encode(blocks, msg):
        exps = jnp.zeros((CODE_ROWS, pw), jnp.float32)
        for i, v in enumerate(blocks):
            most = jnp.max(jnp.abs(v), axis=0, keepdims=True)
            e = jnp.ceil(jnp.log2(jnp.maximum(most, 1e-30)))
            exps = jnp.where(exp_row == i, e, exps)
            q = jnp.clip(jnp.round(v * jnp.exp2(CODE_BITS - e)), -CODE_MOST, CODE_MOST)
            msg[pl.ds(i * half_rows, half_rows), :] = q.astype(jnp.int32).astype(jnp.int16)
        msg[pl.ds(len(blocks) * half_rows, CODE_ROWS), :] = exps.astype(jnp.int32).astype(jnp.int16)

    def decode(msg, n):
        exps = msg[pl.ds(n * half_rows, CODE_ROWS), :].astype(jnp.int32).astype(jnp.float32)
        step = jnp.exp2(exps - CODE_BITS)
        out = []
        for i in range(n):
            q = msg[pl.ds(i * half_rows, half_rows), :].astype(jnp.int32).astype(jnp.float32)
            out.append(q * step[i:i + 1, :])
        return out

    def way(p):
        return (yn, xn) if p % 2 == 0 else (xn, yn)

    h1, h2, h3, h4 = {}, {}, {}, {}
    side = nz * half_rows

    def stage1(q):
        scale_cross(q)
        val = jnp.dot(xt[...], dbuf[:, pl.ds(2 * q * pw, 2 * pw)], preferred_element_type=jnp.float32)
        for p in (2 * q, 2 * q + 1):
            v = val[:, (p % 2) * pw:(p % 2 + 1) * pw]
            keep, give = ((0, 1), (2, 3)) if p % 2 == 0 else ((0, 2), (1, 3))
            out = [v[c * side + z_ * half_rows:c * side + (z_ + 1) * half_rows, :] for c in give for z_ in range(nz)]
            encode(out, q1.at[p])
            h1[p] = send(q1.at[p], r1.at[p], way(p)[0])
            for i, c in enumerate(keep):
                tw[p, i] = v[c * side:(c + 1) * side, :]

    def stage2(q):
        for p in (2 * q, 2 * q + 1):
            h1[p].wait_recv()
            got = decode(r1.at[p], 2 * nz)
            encode([tw[p, 1, pl.ds(z_ * half_rows, half_rows), :] + got[nz + z_] for z_ in range(nz)], q2.at[p])
            h2[p] = send(q2.at[p], r2.at[p], way(p)[1])
            for z_ in range(nz):
                s1[p, z_] = tw[p, 0, pl.ds(z_ * half_rows, half_rows), :] + got[z_]

    def stage3(q):
        for p in (2 * q, 2 * q + 1):
            h2[p].wait_recv()
            for z_, v in enumerate(decode(r2.at[p], nz)):
                tt[p, z_] = s1[p, z_] + v
        for z_ in range(nz):
            encode([tt[2 * q, z_], tt[2 * q + 1, z_]], q3.at[q, z_])
        h3[q] = []
        for k in range(1, nz):
            to = lax.rem(z + k, nz)
            h3[q].append(send(q3.at[q, to], r3.at[q, k - 1], at(g, to, x, core)))

    def stage4(q):
        totals = [tt[2 * q, z], tt[2 * q + 1, z]]
        for k in range(nz - 1):
            h3[q][k].wait_recv()
            totals = [t + v for t, v in zip(totals, decode(r3.at[q, k], 2))]
        for i, total in enumerate(totals):
            p = 2 * q + i
            fin[q, :, pl.ds(i * pw, pw)] = total
            out_ref[pl.ds(pl.multiple_of(g * half_rows, half_rows), half_rows), pl.ds(p * pw, pw)] = total
        h4[q] = send(fin.at[q], r4.at[q], yn)

    cz = []

    def small(n):
        if n == 0:
            cz.pop().wait_recv()
            sb[1] = sb[0] + rb[0]
            cz.append(send(sb.at[1], rb.at[1], xn))
        elif n == 1:
            cz.pop().wait_recv()
            sb[2] = sb[1] + rb[1]
            cz.append(send(sb.at[2], rb.at[2], yn))
        elif n == 2:
            cz.pop().wait_recv()
            sb[3] = sb[2] + rb[2]
            rz[z] = sb[3]
            for k in range(1, nz):
                to = lax.rem(z + k, nz)
                cz.append(send(sb.at[3], rz.at[z], at(g, to, x, core)))

    for stage, q in PLAN:
        if stage == 0:
            if q == 0:
                small_terms()
                cz.append(send(sb.at[0], rb.at[0], partner))
            else:
                small(q - 1)
        else:
            (stage1, stage2, stage3, stage4)[stage - 1](q)
    for cp in cz:
        cp.wait_recv()
    total = rz[0]
    for k in range(1, nz):
        total = total + rz[k]
    small_ref[...] = total
    for q in range(PAIRS):
        h4[q].wait_recv()
        out_ref[pl.ds(pl.multiple_of((1 - g) * half_rows, half_rows), half_rows), pl.ds(2 * q * pw, 2 * pw)] = r4[q]
    for cp in sends:
        cp.wait_send()

    for kind, some in ((is_mid, mid_sends), (is_end, end_sends)):
        @pl.when(kind)
        def _(some=some):
            for i in some:
                pltpu.make_async_remote_copy(
                    src_ref=piece(0, 0, 0, 0), dst_ref=piece(0, 0, 0, 0), send_sem=ssem.at[i], recv_sem=wsem.at[0],
                    device_id=partner, device_id_type=MESH
                ).wait_send()


def shards_fused(
    teacher_rows,
    student_rows,
    counts,
    teacher_weight,
    teacher_bias,
    teacher_gain,
    teacher_head,
    cross_weight,
    cross_bias,
    out_weight,
):
    row_count, fin_width = teacher_rows.shape
    width_s = cross_weight.shape[0]
    group_count = lax.axis_size("group")
    fsdp_count = lax.axis_size("fsdp")
    loss_scale = math.sqrt(width_s / (row_count * group_count * fsdp_count))
    rt = row_count // LANES
    rp = -(-rt // 8) * 8
    nz = fsdp_count // 4
    block = width_s // fsdp_count
    half_rows = block // 2
    parts = 2 * PAIRS
    pw = width_s // parts
    slots = 4 * nz
    f32, bf16, i16 = jnp.float32, jnp.bfloat16, jnp.int16
    vm = pltpu.VMEM
    split = lambda v: v.reshape(-1, 1, LANES)
    anyspec = pl.BlockSpec(memory_space=pl.ANY)
    vspec = pl.BlockSpec(memory_space=pltpu.VMEM)
    grad, small = pl.pallas_call(
        functools.partial(fused, fsdp_count, rp, loss_scale),
        out_shape=(jax.ShapeDtypeStruct((block, width_s), f32), jax.ShapeDtypeStruct((8, width_s), f32)),
        in_specs=[anyspec, anyspec, pl.BlockSpec(memory_space=pltpu.SMEM), anyspec, vspec, vspec, vspec, anyspec, vspec, vspec],
        out_specs=(vspec, vspec),
        scratch_shapes=[
            vm((slots, fin_width, LANES), bf16),
            vm((2 * row_count, fin_width), bf16),
            vm((2 * row_count, width_s), bf16),
            vm((width_s, width_s), bf16),
            vm((slots, 2 * row_count, LANES), f32),
            vm((2 * row_count, LANES), f32),
            vm((slots, LANES), f32),
            vm((row_count, width_s), f32),
            vm((4 * rp, LANES), f32),
            vm((4 * rp, LANES), f32),
            vm((2 * rp, LANES), f32),
            vm((2 * rp, LANES), f32),
            vm((2 * rp, LANES), f32),
            vm((2 * rp, LANES), f32),
            vm((width_s // 2, 2 * row_count), bf16),
            vm((2 * row_count, width_s), bf16),
            vm((2 * row_count, LANES), f32),
            vm((parts, 2, nz * half_rows, pw), f32),
            vm((parts, 2 * nz * half_rows + CODE_ROWS, pw), i16),
            vm((parts, 2 * nz * half_rows + CODE_ROWS, pw), i16),
            vm((parts, nz, half_rows, pw), f32),
            vm((parts, nz * half_rows + CODE_ROWS, pw), i16),
            vm((parts, nz * half_rows + CODE_ROWS, pw), i16),
            vm((parts, nz, half_rows, pw), f32),
            vm((PAIRS, nz, 2 * half_rows + CODE_ROWS, pw), i16),
            vm((PAIRS, nz - 1, 2 * half_rows + CODE_ROWS, pw), i16),
            vm((PAIRS, half_rows, 2 * pw), f32),
            vm((PAIRS, half_rows, 2 * pw), f32),
            vm((4, 8, width_s), f32),
            vm((3, 8, width_s), f32),
            vm((nz, 8, width_s), f32),
            pltpu.SemaphoreType.DMA((4,)),
            pltpu.SemaphoreType.DMA((SENDS,)),
            pltpu.SemaphoreType.DMA((OTHERS,)),
            pltpu.SemaphoreType.DMA((slots * QUARTERS,)),
        ],
        compiler_params=pltpu.CompilerParams(
            collective_id=0, has_side_effects=True, vmem_limit_bytes=60 * 1024 * 1024
        ),
    )(
        teacher_rows, student_rows, counts, teacher_weight, split(teacher_bias), split(teacher_gain),
        split(teacher_head), cross_weight, cross_bias[None, :], out_weight[None, :],
    )
    return (grad, small[0], small[1])


SENDS = 160
OTHERS = 72


def fits(mesh, args):
    rows, fin_width = args[0].shape
    width_s = args[1].shape[1]
    units = args[3].shape[1]
    group_count, fsdp_count = mesh.shape["group"], mesh.shape["fsdp"]
    devices = group_count * fsdp_count
    return (
        group_count == 2
        and fsdp_count == 16
        and units == devices * LANES
        and (rows // devices) % LANES == 0
        and (2 * width_s // fsdp_count) % LANES == 0
        and width_s == 2 * PAIRS * LANES
    )


def solution(mesh):
    in_specs = (
        P(("group", "fsdp"), None),
        P(("group", "fsdp"), None),
        P(("group", "fsdp")),
        P(None, ("group", "fsdp")),
        P(),
        P(),
        P(),
        P(),
        P(),
        P(),
    )
    out_specs = (P("fsdp", None), P(), P())

    def run(*args):
        body = shards_fused if fits(mesh, args) else shards
        return jax.shard_map(body, mesh=mesh, in_specs=in_specs, out_specs=out_specs, check_vma=False)(*args)

    return run
```

```python
import functools
import math

import jax
import jax.numpy as jnp
from jax import lax
from jax.experimental import pallas as pl
from jax.experimental.pallas import tpu as pltpu
from jax.sharding import PartitionSpec as P

epsilon = 1e-06


def shards(
    teacher_rows,
    student_rows,
    counts,
    teacher_weight,
    teacher_bias,
    teacher_gain,
    teacher_head,
    cross_weight,
    cross_bias,
    out_weight,
):
    row_count = teacher_rows.shape[0]
    width_s = cross_weight.shape[0]
    group_count = lax.axis_size("group")
    fsdp_count = lax.axis_size("fsdp")
    shard_count = group_count * fsdp_count
    loss_scale = math.sqrt(width_s / (row_count * shard_count))
    preact = jnp.dot(
        teacher_rows,
        lax.all_gather(teacher_weight, ("group", "fsdp"), axis=1, tiled=True),
        preferred_element_type=jnp.float32,
    )
    preact = preact + teacher_bias
    meansq = jnp.mean(preact * preact, axis=-1, keepdims=True)
    normed = preact * lax.rsqrt(meansq + epsilon) * teacher_gain
    teacher_logit = jnp.sum(jax.nn.silu(normed) * teacher_head, axis=-1)
    cross = jnp.dot(student_rows, cross_weight, preferred_element_type=jnp.float32) + cross_bias
    inputs_f = student_rows.astype(jnp.float32)
    mixed = inputs_f * cross + inputs_f
    student_logit = jnp.sum(mixed * out_weight, axis=-1)
    live_rows = (jnp.arange(row_count, dtype=jnp.int32) < counts[0]).astype(jnp.float32)
    error = (student_logit - teacher_logit) * live_rows * loss_scale
    dcross = error[:, None] * out_weight[None, :] * inputs_f
    dcross_half = dcross.astype(jnp.bfloat16)
    term_b = jnp.sum(dcross, axis=0)
    term_o = jnp.sum(error[:, None] * mixed, axis=0)
    term_w = lax.dot_general(
        student_rows, dcross_half, (((0,), (0,)), ((), ())), preferred_element_type=jnp.float32
    )
    totals = lax.psum((term_w, term_b, term_o), "group")
    grad_cross = lax.psum_scatter(totals[0], "fsdp", scatter_dimension=0, tiled=True)
    small_sums = lax.psum((totals[1], totals[2]), "fsdp")
    return (grad_cross, small_sums[0], small_sums[1])


MESH = pl.DeviceIdType.MESH
LANES = 128
PAIRS = 4
QUARTERS = 4
CODE_ROWS = 16
CODE_BITS = 15.0
CODE_MOST = 32767.0
PLAN = (
    (1, 0), (1, 1), (1, 2), (2, 0), (1, 3), (0, 0), (2, 1), (3, 0), (0, 1), (2, 2), (3, 1), (0, 2), (2, 3), (3, 2), (4, 0), (0, 3),
    (3, 3), (4, 1), (4, 2), (4, 3),
)


def fused(fsdp_count, rp, loss_scale, t_ref, s_ref, count_ref, w_ref, bias_ref, gain_ref, head_ref, cw_ref, cb_ref, ow_ref,
          out_ref, small_ref,
          wbuf, rows, xs, cw, pre, ssq, heads, mixed, msg1, in1, msg2, in2, rr, er, xt, dbuf,
          ecol, tw, q1, r1, s1, q2, r2, tt, q3, r3, fin, r4, sb, rb, rz, lsem, ssem, rsem, wsem):
    g = lax.axis_index("group")
    f = lax.axis_index("fsdp")
    core = lax.rem(f, 2)
    x = lax.rem(lax.div(f, 2), 2)
    z = lax.div(f, 4)
    nz = fsdp_count // 4
    row_count, fin_width = t_ref.shape
    width_s = s_ref.shape[1]
    block = width_s // fsdp_count
    half_rows = block // 2
    rt = row_count // LANES
    units = bias_ref.shape[0] * LANES
    parts = 2 * PAIRS
    pw = width_s // parts

    def at(y_, z_, x_, c_):
        return (y_, (z_ * 2 + x_) * 2 + c_)

    partner = at(g, z, x, 1 - core)
    xn = at(g, z, 1 - x, core)
    yn = at(1 - g, z, x, core)
    barrier = pltpu.get_barrier_semaphore()
    peers = [partner, xn, yn] + [at(g, lax.rem(z + k, nz), x, core) for k in range(1, nz)]
    for peer in peers:
        pl.semaphore_signal(barrier, inc=1, device_id=peer, device_id_type=MESH)

    locals_ = []
    for i, (a, b) in enumerate([
        (s_ref, xs.at[pl.ds(0, row_count)]),
        (cw_ref, cw),
        (w_ref, wbuf.at[0]),
        (t_ref, rows.at[pl.ds(0, row_count)]),
    ]):
        cp = pltpu.make_async_copy(a, b, lsem.at[i])
        cp.start()
        locals_.append(cp)
    pl.semaphore_wait(barrier, len(peers))

    sends = []
    mid_sends = []
    end_sends = []
    waits = []
    turn = [0]

    def send(a, b, device, recv=None, only=None):
        i = turn[0]
        turn[0] += 1
        if recv is None:
            recv = rsem.at[len(waits)]
            waits.append(i)
        cp = pltpu.make_async_remote_copy(
            src_ref=a, dst_ref=b, send_sem=ssem.at[i], recv_sem=recv, device_id=device, device_id_type=MESH
        )
        cp.start()
        if only:
            (end_sends if only == 'end' else mid_sends).append(i)
        else:
            sends.append(cp)
        return cp

    half_z = lax.div(z, 2)
    is_mid = jnp.logical_or(z == 1, z == 2)
    is_end = jnp.logical_not(is_mid)
    plane = (z, z + 1 - 2 * lax.rem(z, 2), 2 - half_z, 3 - 3 * half_z)
    zpair = at(g, plane[1], x, core)
    zmid = at(g, nz - 1 - z, x, core)
    depth = fin_width // QUARTERS
    quarters = list(range(QUARTERS))
    first, last = quarters[:QUARTERS // 2], quarters[QUARTERS // 2:]

    def slot(dx, dy, n):
        return (dx * 2 + dy) * nz + n

    def piece(dx, dy, n, q):
        return wbuf.at[slot(dx, dy, n), pl.ds(q * depth, depth)]

    def arrival(dx, dy, n, q):
        return wsem.at[slot(dx, dy, n) * QUARTERS + q]

    def pass_on(src, dst, q, device, only=None):
        here = w_ref.at[pl.ds(q * depth, depth)] if src is None else piece(*src, q)
        send(here, piece(*dst, q), device, arrival(*dst, q), only)

    def landed(dx, dy, n, qs):
        for q in qs:
            pltpu.make_async_remote_copy(
                src_ref=piece(dx, dy, n, q), dst_ref=piece(dx, dy, n, q), send_sem=ssem.at[0],
                recv_sem=arrival(dx, dy, n, q), device_id=partner, device_id_type=MESH
            ).wait_recv()

    def sideways(src, n):
        for qx, qy in zip(last + first, quarters):
            pass_on(src, (1, 0, n), qx, xn)
            pass_on(src, (0, 1, n), qy, yn)

    for qx, q in zip(last + first, quarters):
        pass_on(None, (1, 0, 0), qx, xn)
        pass_on(None, (0, 1, 0), q, yn)
        pass_on(None, (0, 0, 1), q, zpair)

    @pl.when(is_mid)
    def _():
        for q in quarters:
            pass_on(None, (0, 0, 2), q, zmid, 'mid')

    rows_in = send(t_ref, rows.at[pl.ds(row_count, row_count)], partner)
    xs_in = send(s_ref, xs.at[pl.ds(row_count, row_count)], partner)

    def diagonal(n):
        for qx, qy in zip(first, last):
            landed(0, 1, n, [qx])
            pass_on((0, 1, n), (1, 1, n), qx, xn)
            landed(1, 0, n, [qy])
            pass_on((1, 0, n), (1, 1, n), qy, yn)

    def rest(n):
        landed(0, 1, n, last)
        landed(1, 0, n, first)

    eye = lax.broadcasted_iota(jnp.int32, (LANES, LANES), 0) == lax.broadcasted_iota(jnp.int32, (LANES, LANES), 1)

    def to_row(col):
        return jnp.sum(jnp.where(eye, col, 0.0), axis=0, keepdims=True)

    def to_col(row):
        return jnp.sum(jnp.where(eye, row, 0.0), axis=1, keepdims=True)

    def tile(t):
        return pl.ds(pl.multiple_of(t * LANES, LANES), LANES)

    ssq[...] = jnp.zeros_like(ssq)
    for ref in (msg1, msg2, er, rr):
        ref[...] = jnp.zeros_like(ref)
    row = lax.broadcasted_iota(jnp.int32, (rt, LANES), 0) * LANES + lax.broadcasted_iota(jnp.int32, (rt, LANES), 1)
    msg1[pl.ds(3 * rp, rt), :] = jnp.where(row < count_ref[0], loss_scale, 0.0)

    locals_[0].wait()
    locals_[1].wait()
    ow = ow_ref[...]

    def student(t, carry):
        xt_ = xs[tile(t), :]
        cross = jnp.dot(xt_, cw[...], preferred_element_type=jnp.float32) + cb_ref[...]
        xf = xt_.astype(jnp.float32)
        m = xf * cross + xf
        mixed[tile(t), :] = m
        msg1[pl.ds(2 * rp + t, 1), :] = to_row(jnp.sum(m * ow, axis=1, keepdims=True))
        return carry

    lax.fori_loop(0, rt, student, 0)
    locals_[2].wait()
    locals_[3].wait()

    mt = row_count

    def column_block(dx, dy, n):
        y_ = g if dy == 0 else 1 - g
        x_ = x if dx == 0 else 1 - x
        return y_ * fsdp_count + (plane[n] * 2 + x_) * 2 + core

    def project(*blocks):
        found = []
        for b_ in blocks:
            index = column_block(*b_)
            heads[pl.ds(slot(*b_), 1), :] = head_ref[index]
            found.append((slot(*b_), gain_ref[index] * 0.5, bias_ref[index]))

        def step(t, carry):
            ds = pl.ds(pl.multiple_of(t * mt, mt), mt)
            w = jnp.concatenate([wbuf[s] for s, _, _ in found], axis=1) if len(found) > 1 else wbuf[found[0][0]]
            both = jnp.dot(rows[ds, :], w, preferred_element_type=jnp.float32)
            for i, (s, gain, bias) in enumerate(found):
                p = both[:, i * LANES:(i + 1) * LANES] + bias
                pre[s, ds, :] = p * gain
                ssq[ds, :] += p * p
            return carry

        lax.fori_loop(0, 2 * row_count // mt, step, 0)

    order = [q for pair in zip(first, last) for q in pair]

    for i, (qx, qy) in enumerate(zip(first, last)):
        landed(0, 1, 0, [qx])
        pass_on((0, 1, 0), (1, 1, 0), qx, xn)
        landed(1, 0, 0, [qy])
        pass_on((1, 0, 0), (1, 1, 0), qy, yn)

        @pl.when(is_mid)
        def _(i=i):
            for q in quarters[2 * i:2 * i + 2]:
                landed(0, 0, 2, [q])
                pass_on((0, 0, 2), (0, 0, 2), q, zpair, 'mid')
                landed(0, 0, 1, [q])
                pass_on((0, 0, 1), (0, 0, 3), q, zmid, 'mid')

    rows_in.wait_recv()
    project((0, 0, 0))

    @pl.when(is_end)
    def _():
        landed(0, 0, 1, quarters)

    sideways((0, 0, 1), 1)
    rest(0)
    project((1, 0, 0))

    def far(q):
        landed(0, 0, 3, [q])
        pass_on((0, 0, 3), (0, 0, 3), q, zpair, 'mid')

    @pl.when(is_mid)
    def _():
        far(0)

    project((0, 1, 0))
    for i, q in enumerate(order):
        landed(1, 1, 0, [q])

        @pl.when(is_end)
        def _(q=q):
            pass_on((1, 1, 0), (1, 1, 1), q, zpair, 'end')

        @pl.when(is_mid)
        def _(q=q, i=i):
            pass_on((1, 1, 0), (1, 1, 2), q, zmid, 'mid')
            if i == 1:
                far(1)

    project((0, 0, 1))
    xs_in.wait_recv()
    pick = (
        lax.broadcasted_iota(jnp.int32, (block, 2 * block), 1)
        == lax.broadcasted_iota(jnp.int32, (block, 2 * block), 0) + core * block
    )
    pick = jnp.where(pick, 1.0, 0.0).astype(jnp.bfloat16)
    for j in range(fsdp_count // 2):
        turned = lax.dot_general(
            pick, xs[:, pl.ds(j * 2 * block, 2 * block)], (((1,), (1,)), ((), ())), preferred_element_type=jnp.float32
        ).astype(jnp.bfloat16)
        far_x = lax.rem(x + j % 2, 2)
        for y_ in range(2):
            to = ((lax.rem(g + y_, 2) * 2 + far_x) * nz + j // 2) * half_rows
            xt[pl.ds(pl.multiple_of(to, half_rows), half_rows), :] = turned[y_ * half_rows:(y_ + 1) * half_rows, :]

    @pl.when(is_mid)
    def _():
        for q in quarters[2:]:
            far(q)
        for q in order:
            pass_on((1, 1, 0), (1, 1, 1), q, zpair, 'mid')

    @pl.when(is_end)
    def _():
        landed(0, 0, 2, quarters)

    sideways((0, 0, 2), 2)
    project((1, 1, 0))
    project((0, 0, 2))
    landed(1, 0, 1, quarters)
    project((1, 0, 1))
    landed(0, 1, 1, quarters)

    @pl.when(is_end)
    def _():
        landed(0, 0, 3, quarters)

    sideways((0, 0, 3), 3)
    project((0, 1, 1))

    @pl.when(is_mid)
    def _():
        for q in order:
            landed(1, 1, 2, [q])
            pass_on((1, 1, 2), (1, 1, 2), q, zpair, 'mid')

    project((0, 0, 3))
    for at_ in ((1, 0, 2), (0, 1, 2)):
        landed(*at_, quarters)
        project(at_)
    diagonal(3)
    landed(1, 1, 1, quarters)
    project((1, 1, 1))
    rest(3)
    project((1, 0, 3))
    project((0, 1, 3))

    @pl.when(is_end)
    def _():
        landed(1, 1, 2, quarters)

    landed(1, 1, 3, quarters)
    project((1, 1, 2), (1, 1, 3))

    for h in range(2):
        def squares(t, carry, h=h):
            col = jnp.sum(ssq[tile(h * rt + t), :], axis=1, keepdims=True)
            msg1[pl.ds(h * rp + t, 1), :] = to_row(col)
            return carry

        lax.fori_loop(0, rt, squares, 0, unroll=True)
    m1 = send(msg1, in1, partner)
    m1.wait_recv()
    for h in range(2):
        total = msg1[pl.ds(h * rp, rp), :] + in1[pl.ds((1 - h) * rp, rp), :]
        rr[pl.ds(h * rp, rp), :] = lax.rsqrt(total * (1.0 / units) + epsilon)

    for h in range(2):
        def logits(t, carry, h=h):
            r = to_col(rr[pl.ds(h * rp + t, 1), :])
            acc = jnp.zeros((LANES, LANES), jnp.float32)
            for s in range(4 * nz):
                v = pre[s, tile(h * rt + t), :] * r
                acc += (v * jnp.tanh(v) + v) * heads[pl.ds(s, 1), :]
            msg2[pl.ds(h * rp + t, 1), :] = to_row(jnp.sum(acc, axis=1, keepdims=True))
            return carry

        lax.fori_loop(0, rt, logits, 0)
    m2 = send(msg2, in2, partner)
    m2.wait_recv()
    for h, src in ((0, msg1), (1, in1)):
        teacher = msg2[pl.ds(h * rp, rp), :] + in2[pl.ds((1 - h) * rp, rp), :]
        er[pl.ds(h * rp, rp), :] = (src[pl.ds(2 * rp, rp), :] - teacher) * src[pl.ds(3 * rp, rp), :]

    def spread(t, carry):
        ecol[tile(t), :] = jnp.broadcast_to(to_col(er[pl.ds(t, 1), :]), (LANES, LANES))
        ecol[tile(rt + t), :] = jnp.broadcast_to(to_col(er[pl.ds(rp + t, 1), :]), (LANES, LANES))
        return carry

    lax.fori_loop(0, rt, spread, 0, unroll=True)
    sb[...] = jnp.zeros_like(sb)

    def scale_cross(q):
        cols = pl.ds(2 * q * pw, 2 * pw)
        owp = ow_ref[:, cols]

        def cross_tile(t, carry):
            e = ecol[tile(t), :]
            d = jnp.concatenate([e, e], axis=1) * owp * xs[tile(t), cols].astype(jnp.float32)
            dbuf[tile(t), cols] = d.astype(jnp.bfloat16)
            return carry

        lax.fori_loop(0, 2 * rt, cross_tile, 0, unroll=2)

    def small_terms():
        def one(t, carry):
            for p in range(parts):
                cols = pl.ds(p * pw, pw)
                e = ecol[tile(t), :]
                d = e * ow_ref[:, cols] * xs[tile(t), cols].astype(jnp.float32)
                sb[0, pl.ds(0, 1), cols] += jnp.sum(d, axis=0, keepdims=True)
                sb[0, pl.ds(1, 1), cols] += jnp.sum(e * mixed[tile(t), cols], axis=0, keepdims=True)
            return carry

        lax.fori_loop(0, rt, one, 0)

    exp_row = lax.broadcasted_iota(jnp.int32, (CODE_ROWS, pw), 0)

    def encode(blocks, msg):
        exps = jnp.zeros((CODE_ROWS, pw), jnp.float32)
        for i, v in enumerate(blocks):
            most = jnp.max(jnp.abs(v), axis=0, keepdims=True)
            e = jnp.ceil(jnp.log2(jnp.maximum(most, 1e-30)))
            exps = jnp.where(exp_row == i, e, exps)
            q = jnp.clip(jnp.round(v * jnp.exp2(CODE_BITS - e)), -CODE_MOST, CODE_MOST)
            msg[pl.ds(i * half_rows, half_rows), :] = q.astype(jnp.int32).astype(jnp.int16)
        msg[pl.ds(len(blocks) * half_rows, CODE_ROWS), :] = exps.astype(jnp.int32).astype(jnp.int16)

    def decode(msg, n):
        exps = msg[pl.ds(n * half_rows, CODE_ROWS), :].astype(jnp.int32).astype(jnp.float32)
        step = jnp.exp2(exps - CODE_BITS)
        out = []
        for i in range(n):
            q = msg[pl.ds(i * half_rows, half_rows), :].astype(jnp.int32).astype(jnp.float32)
            out.append(q * step[i:i + 1, :])
        return out

    def way(p):
        return (yn, xn) if p % 2 == 0 else (xn, yn)

    h1, h2, h3, h4 = {}, {}, {}, {}
    side = nz * half_rows

    def stage1(q):
        scale_cross(q)
        val = jnp.dot(xt[...], dbuf[:, pl.ds(2 * q * pw, 2 * pw)], preferred_element_type=jnp.float32)
        for p in (2 * q, 2 * q + 1):
            v = val[:, (p % 2) * pw:(p % 2 + 1) * pw]
            keep, give = ((0, 1), (2, 3)) if p % 2 == 0 else ((0, 2), (1, 3))
            out = [v[c * side + z_ * half_rows:c * side + (z_ + 1) * half_rows, :] for c in give for z_ in range(nz)]
            encode(out, q1.at[p])
            h1[p] = send(q1.at[p], r1.at[p], way(p)[0])
            for i, c in enumerate(keep):
                tw[p, i] = v[c * side:(c + 1) * side, :]

    def stage2(q):
        for p in (2 * q, 2 * q + 1):
            h1[p].wait_recv()
            got = decode(r1.at[p], 2 * nz)
            encode([tw[p, 1, pl.ds(z_ * half_rows, half_rows), :] + got[nz + z_] for z_ in range(nz)], q2.at[p])
            h2[p] = send(q2.at[p], r2.at[p], way(p)[1])
            for z_ in range(nz):
                s1[p, z_] = tw[p, 0, pl.ds(z_ * half_rows, half_rows), :] + got[z_]

    def stage3(q):
        for p in (2 * q, 2 * q + 1):
            h2[p].wait_recv()
            for z_, v in enumerate(decode(r2.at[p], nz)):
                tt[p, z_] = s1[p, z_] + v
        for z_ in range(nz):
            encode([tt[2 * q, z_], tt[2 * q + 1, z_]], q3.at[q, z_])
        h3[q] = []
        for k in range(1, nz):
            to = lax.rem(z + k, nz)
            h3[q].append(send(q3.at[q, to], r3.at[q, k - 1], at(g, to, x, core)))

    def stage4(q):
        totals = [tt[2 * q, z], tt[2 * q + 1, z]]
        for k in range(nz - 1):
            h3[q][k].wait_recv()
            totals = [t + v for t, v in zip(totals, decode(r3.at[q, k], 2))]
        for i, total in enumerate(totals):
            p = 2 * q + i
            fin[q, :, pl.ds(i * pw, pw)] = total
            out_ref[pl.ds(pl.multiple_of(g * half_rows, half_rows), half_rows), pl.ds(p * pw, pw)] = total
        h4[q] = send(fin.at[q], r4.at[q], yn)

    cz = []

    def small(n):
        if n == 0:
            cz.pop().wait_recv()
            sb[1] = sb[0] + rb[0]
            cz.append(send(sb.at[1], rb.at[1], xn))
        elif n == 1:
            cz.pop().wait_recv()
            sb[2] = sb[1] + rb[1]
            cz.append(send(sb.at[2], rb.at[2], yn))
        elif n == 2:
            cz.pop().wait_recv()
            sb[3] = sb[2] + rb[2]
            rz[z] = sb[3]
            for k in range(1, nz):
                to = lax.rem(z + k, nz)
                cz.append(send(sb.at[3], rz.at[z], at(g, to, x, core)))

    for stage, q in PLAN:
        if stage == 0:
            if q == 0:
                small_terms()
                cz.append(send(sb.at[0], rb.at[0], partner))
            else:
                small(q - 1)
        else:
            (stage1, stage2, stage3, stage4)[stage - 1](q)
    for cp in cz:
        cp.wait_recv()
    total = rz[0]
    for k in range(1, nz):
        total = total + rz[k]
    small_ref[...] = total
    for q in range(PAIRS):
        h4[q].wait_recv()
        out_ref[pl.ds(pl.multiple_of((1 - g) * half_rows, half_rows), half_rows), pl.ds(2 * q * pw, 2 * pw)] = r4[q]
    for cp in sends:
        cp.wait_send()

    for kind, some in ((is_mid, mid_sends), (is_end, end_sends)):
        @pl.when(kind)
        def _(some=some):
            for i in some:
                pltpu.make_async_remote_copy(
                    src_ref=piece(0, 0, 0, 0), dst_ref=piece(0, 0, 0, 0), send_sem=ssem.at[i], recv_sem=wsem.at[0],
                    device_id=partner, device_id_type=MESH
                ).wait_send()


def shards_fused(
    teacher_rows,
    student_rows,
    counts,
    teacher_weight,
    teacher_bias,
    teacher_gain,
    teacher_head,
    cross_weight,
    cross_bias,
    out_weight,
):
    row_count, fin_width = teacher_rows.shape
    width_s = cross_weight.shape[0]
    group_count = lax.axis_size("group")
    fsdp_count = lax.axis_size("fsdp")
    loss_scale = math.sqrt(width_s / (row_count * group_count * fsdp_count))
    rt = row_count // LANES
    rp = -(-rt // 8) * 8
    nz = fsdp_count // 4
    block = width_s // fsdp_count
    half_rows = block // 2
    parts = 2 * PAIRS
    pw = width_s // parts
    slots = 4 * nz
    f32, bf16, i16 = jnp.float32, jnp.bfloat16, jnp.int16
    vm = pltpu.VMEM
    split = lambda v: v.reshape(-1, 1, LANES)
    anyspec = pl.BlockSpec(memory_space=pl.ANY)
    vspec = pl.BlockSpec(memory_space=pltpu.VMEM)
    grad, small = pl.pallas_call(
        functools.partial(fused, fsdp_count, rp, loss_scale),
        out_shape=(jax.ShapeDtypeStruct((block, width_s), f32), jax.ShapeDtypeStruct((8, width_s), f32)),
        in_specs=[anyspec, anyspec, pl.BlockSpec(memory_space=pltpu.SMEM), anyspec, vspec, vspec, vspec, anyspec, vspec, vspec],
        out_specs=(vspec, vspec),
        scratch_shapes=[
            vm((slots, fin_width, LANES), bf16),
            vm((2 * row_count, fin_width), bf16),
            vm((2 * row_count, width_s), bf16),
            vm((width_s, width_s), bf16),
            vm((slots, 2 * row_count, LANES), f32),
            vm((2 * row_count, LANES), f32),
            vm((slots, LANES), f32),
            vm((row_count, width_s), f32),
            vm((4 * rp, LANES), f32),
            vm((4 * rp, LANES), f32),
            vm((2 * rp, LANES), f32),
            vm((2 * rp, LANES), f32),
            vm((2 * rp, LANES), f32),
            vm((2 * rp, LANES), f32),
            vm((width_s // 2, 2 * row_count), bf16),
            vm((2 * row_count, width_s), bf16),
            vm((2 * row_count, LANES), f32),
            vm((parts, 2, nz * half_rows, pw), f32),
            vm((parts, 2 * nz * half_rows + CODE_ROWS, pw), i16),
            vm((parts, 2 * nz * half_rows + CODE_ROWS, pw), i16),
            vm((parts, nz, half_rows, pw), f32),
            vm((parts, nz * half_rows + CODE_ROWS, pw), i16),
            vm((parts, nz * half_rows + CODE_ROWS, pw), i16),
            vm((parts, nz, half_rows, pw), f32),
            vm((PAIRS, nz, 2 * half_rows + CODE_ROWS, pw), i16),
            vm((PAIRS, nz - 1, 2 * half_rows + CODE_ROWS, pw), i16),
            vm((PAIRS, half_rows, 2 * pw), f32),
            vm((PAIRS, half_rows, 2 * pw), f32),
            vm((4, 8, width_s), f32),
            vm((3, 8, width_s), f32),
            vm((nz, 8, width_s), f32),
            pltpu.SemaphoreType.DMA((4,)),
            pltpu.SemaphoreType.DMA((SENDS,)),
            pltpu.SemaphoreType.DMA((OTHERS,)),
            pltpu.SemaphoreType.DMA((slots * QUARTERS,)),
        ],
        compiler_params=pltpu.CompilerParams(
            collective_id=0, has_side_effects=True, vmem_limit_bytes=60 * 1024 * 1024
        ),
    )(
        teacher_rows, student_rows, counts, teacher_weight, split(teacher_bias), split(teacher_gain),
        split(teacher_head), cross_weight, cross_bias[None, :], out_weight[None, :],
    )
    return (grad, small[0], small[1])


SENDS = 160
OTHERS = 72


def fits(mesh, args):
    rows, fin_width = args[0].shape
    width_s = args[1].shape[1]
    units = args[3].shape[1]
    group_count, fsdp_count = mesh.shape["group"], mesh.shape["fsdp"]
    devices = group_count * fsdp_count
    return (
        group_count == 2
        and fsdp_count == 16
        and units == devices * LANES
        and (rows // devices) % LANES == 0
        and (2 * width_s // fsdp_count) % LANES == 0
        and width_s == 2 * PAIRS * LANES
    )


def solution(mesh):
    in_specs = (
        P(("group", "fsdp"), None),
        P(("group", "fsdp"), None),
        P(("group", "fsdp")),
        P(None, ("group", "fsdp")),
        P(),
        P(),
        P(),
        P(),
        P(),
        P(),
    )
    out_specs = (P("fsdp", None), P(), P())

    def run(*args):
        body = shards_fused if fits(mesh, args) else shards
        return jax.shard_map(body, mesh=mesh, in_specs=in_specs, out_specs=out_specs, check_vma=False)(*args)

    return run
```
